32 devices in a mesh: grp: 2 (over y), seq: 4 (over z), head: 2 (over x), rep: 2 (over core).
Axes of the slice: x: 2, y: 2, z: 4, core: 2. Of those that a mesh axis runs over, the one named last changes fastest.
Arguments:
- x_proj: bfloat16 [4, 4, 4, 32, 8192], P(('grp', 'rep'), None, 'seq', None, 'head'), parts along dimension 0, may hold values from -6 to 6
- gate_proj: bfloat16 [4, 4, 4, 32, 8192], P(('grp', 'rep'), None, 'seq', None, 'head'), parts along dimension 0, may hold values from -6 to 6
- bc_proj: bfloat16 [4, 4, 4, 32, 256], P(('grp', 'rep'), None, 'seq'), parts along dimension 0, may hold values from -6 to 6
- dt_proj: bfloat16 [4, 4, 4, 32, 128], P(('grp', 'rep'), None, 'seq', None, 'head'), parts along dimension 0, may hold values from -5.5 to 7.5
- a_rate: float32 [128], P('head'), may hold values from 0.0001953125 to 0.05
- dt_bias: float32 [128], P('head'), may hold values from -1 to 1
- d_skip: float32 [128], P('head'), may hold values from 0.5 to 1.5
- conv_x_weight: float32 [4, 8192], P(None, 'head'), may hold values from -3 to 3
- conv_bc_weight: float32 [4, 256], replicated, may hold values from -3 to 3
- norm_gain: float32 [8192], P('head'), may hold values from 0.1 to 1.9
- out_weight: bfloat16 [8192, 2048], P(('seq', 'rep'), 'head'), may hold values from -0.0625 to 0.0625
- request_first_position: int32 [4], P(('grp', 'rep')), parts along dimension 0, may hold values from 0 to 255
- owner: int32 [4, 4], P(('grp', 'rep')), parts along dimension 0, may hold values from 0 to 3, each once within a row
Outputs:
- mixed: bfloat16 [4, 512, 2048], P(('grp', 'rep'), 'seq', 'head'), parts along dimension 0
- ssm_state: float32 [4, 4, 128, 2048], P(('grp', 'rep'), 'seq', 'head'), parts along dimension 0
- conv_x_state: bfloat16 [4, 4, 3, 2048], P(('grp', 'rep'), 'seq', None, 'head'), parts along dimension 0
- conv_bc_state: bfloat16 [4, 4, 3, 64], P(('grp', 'rep'), 'seq'), parts along dimension 0
The draws below stay inside these ranges and needn't reach their ends.
There are 2 independent parts, one for each index of `grp`. The reference program is written for one: setup_inputs(seed, part) draws one part's arguments, and reference() takes and returns one part's arrays. A program takes and returns all parts, laid end to end along the dimension named above; an argument that names none is the same for every part. Nothing has to cross between parts.
Inputs may be any that keep to these rules, and one draw needn't show every extreme that they name: Each row of owner names every index of seq once.
All inputs are finite; a program needn't handle non-finite values.
Results may differ from the reference program's by a relative error of at most 0.007.
Values may be sent and summed in bfloat16 or wider, within the bound.
A program may use at most 128 MiB of HBM per device.

```python
import jax
import jax.numpy as jnp
from jax import lax

D = 2048
HEADS = 128
HEAD_DIM = 64
NSTATE = 128
KCONV = 4
SPAN = 128
TOK_DEV = 128
INNER = 8192
LENGTH = 512
SUB = 32
REQS = 2
N_SEQ = 4
N_HEAD = 2


def draw_dt_proj(key, part):
    axis_extents = (REQS, N_SEQ, N_SEQ, SUB, HEADS)
    starting_displacement = 0.5 * jnp.clip(jax.random.normal(key, axis_extents, jnp.float32), -3.0, 3.0)
    block_offset = jax.random.uniform(jax.random.fold_in(key, 11), (REQS, N_SEQ, 1, 1, HEADS), jnp.float32, -2.5, 1.5)
    spots = jax.random.randint(jax.random.fold_in(key, 7), (REQS, 3, HEADS), 0, LENGTH)
    agreeing_tally = jnp.arange(LENGTH, dtype=jnp.int32)[None, :, None, None] == spots[:, None, :, :]
    segment_extent = jnp.any(agreeing_tally, axis=2).astype(jnp.float32) * 4.0
    return (starting_displacement + block_offset + segment_extent.reshape(axis_extents)).astype(jnp.bfloat16)


def draw_a_rate(key, part):
    share = 0.5
    picked = jax.random.uniform(jax.random.fold_in(key, 1), (HEADS,), jnp.float32)
    level = jax.random.uniform(jax.random.fold_in(key, 2), (HEADS,), jnp.float32)
    slow_rate = jnp.exp(jnp.log(0.3 / LENGTH) + level * jnp.log(2.0 / 0.3))
    quick_decay_speed = jnp.exp(jnp.log(1.0 / LENGTH) + level * jnp.log(0.05 * LENGTH))
    return jnp.where(picked < share, slow_rate, quick_decay_speed).astype(jnp.float32)


def shard_levels(rng, shape, cuts, least, high):
    loudness, own = 1.0, jax.random.fold_in(rng, 6)
    for dim, shards_of in cuts:
        draws = jnp.exp(jax.random.uniform(jax.random.fold_in(own, dim), (shards_of,), jnp.float32, least / len(cuts), high / len(cuts)))
        loudness = loudness * jnp.repeat(draws, shape[dim] // shards_of).reshape([-1 if axis == dim else 1 for axis in range(len(shape))])
    return loudness


def normal_values(key, dims, width, most, pieces=(), kind=jnp.bfloat16):
    loudness = shard_levels(key, dims, pieces, -0.22, 0.18) if pieces else 1.0
    array = jax.random.normal(key, dims, jnp.float32) * width * loudness
    return jnp.minimum(jnp.maximum(array, -most), most).astype(kind)


def setup_inputs(seed: int = 0, part: int = 0) -> dict:
    streams_of = jax.random.split(jax.random.key(seed), 14)
    part_keys = jax.random.split(jax.random.fold_in(streams_of[13], part), 14)
    x_proj = normal_values(part_keys[0], (REQS, N_SEQ, N_SEQ, SUB, INNER), 1.0, 6.0, ((0, 2), (2, 4), (4, 2)))
    gate_proj = normal_values(part_keys[1], (REQS, N_SEQ, N_SEQ, SUB, INNER), 1.0, 6.0, ((0, 2), (2, 4), (4, 2)))
    bc_proj = normal_values(part_keys[2], (REQS, N_SEQ, N_SEQ, SUB, 2 * NSTATE), 1.0, 6.0, ((0, 2), (2, 4)))
    dt_proj = draw_dt_proj(jax.random.fold_in(jax.random.fold_in(streams_of[13], part), 71), part)
    a_rate = draw_a_rate(jax.random.fold_in(streams_of[13], 71), part)
    dt_bias = jnp.clip(jax.random.uniform(streams_of[5], (HEADS,), jnp.float32, -1.0, 1.0) * shard_levels(streams_of[5], (HEADS,), ((0, 2),), -0.4, 0.0), -1.0, 1.0)
    d_skip = jnp.clip(0.5 + 1.0 * jax.random.uniform(streams_of[6], (HEADS,), jnp.float32) ** shard_levels(streams_of[6], (HEADS,), ((0, 2),), -0.2, 0.2), 0.5, 1.5)
    conv_x_weight = normal_values(streams_of[7], (KCONV, INNER), KCONV ** -0.5, 3.0, ((1, 2),), jnp.float32)
    conv_bc_weight = normal_values(streams_of[8], (KCONV, 2 * NSTATE), KCONV ** -0.5, 3.0, (), jnp.float32)
    norm_gain = jnp.clip(1.0 + 0.18 * jax.random.normal(streams_of[9], (INNER,), jnp.float32), 0.1, 1.9)
    out_weight = normal_values(streams_of[10], (INNER, D), INNER ** -0.5, 0.0625, ((0, 8), (1, 2)))
    request_first_position = jax.random.randint(part_keys[11], (REQS,), 0, LENGTH // 2).astype(jnp.int32)
    owner = jax.vmap(lambda own: jax.random.permutation(own, N_SEQ))(jax.random.split(part_keys[12], REQS)).reshape((REQS, N_SEQ)).astype(jnp.int32)
    return dict(x_proj=x_proj, gate_proj=gate_proj, bc_proj=bc_proj, dt_proj=dt_proj, a_rate=a_rate, dt_bias=dt_bias, d_skip=d_skip, conv_x_weight=conv_x_weight, conv_bc_weight=conv_bc_weight, norm_gain=norm_gain, out_weight=out_weight, request_first_position=request_first_position, owner=owner)


highest = lax.Precision.HIGHEST
stability_constant = 1e-05

def span_terms(x_conv, b_rows, c_rows, step_size, log_decay):
    cum_decay = jnp.cumsum(log_decay, axis=1)
    scores = jnp.einsum('kqn,ktn->kqt', c_rows.astype(jnp.float32), b_rows.astype(jnp.float32), precision=highest)
    cum_heads = jnp.swapaxes(cum_decay, 1, 2)
    step_heads = jnp.swapaxes(step_size, 1, 2)
    block_len = cum_decay.shape[1]
    causal = jnp.arange(block_len)[:, None] >= jnp.arange(block_len)[None, :]
    decay_gap = cum_heads[:, :, :, None] - cum_heads[:, :, None, :]
    seg_decay = jnp.exp(jnp.where(causal, decay_gap, -jnp.inf))
    weights = (scores[:, None] * seg_decay * step_heads[:, :, None, :]).astype(jnp.bfloat16)
    y_intra = jnp.einsum('khqt,kthp->kqhp', weights.astype(jnp.float32), x_conv.astype(jnp.float32), precision=highest)
    remaining_length = jnp.exp(cum_decay[:, -1:, :] - cum_decay)
    scaled = ((remaining_length * step_size)[..., None] * x_conv.astype(jnp.float32)).astype(jnp.bfloat16)
    states = jnp.einsum('kthp,ktn->khpn', scaled.astype(jnp.float32), b_rows.astype(jnp.float32), precision=highest)
    return (cum_decay, y_intra, states, jnp.exp(cum_decay[:, -1, :]))

def conv_silu(values, weight):
    length = values.shape[0]
    padded = jnp.concatenate([jnp.zeros((weight.shape[0] - 1, values.shape[1]), values.dtype), values], axis=0)
    accum = jnp.zeros(values.shape, jnp.float32)
    for offset in range(weight.shape[0]):
        accum = accum + weight[offset] * padded[offset:offset + length].astype(jnp.float32)
    return jax.nn.silu(accum)

def one_request(x_in, z_in, bc_in, dt_in, start, a_rate, dt_bias, d_skip, conv_x_weight, conv_bc_weight, norm_gain, out_weight):
    length = x_in.shape[0]
    is_live = jnp.arange(length, dtype=jnp.int32) >= start
    x_live = jnp.where(is_live[:, None], x_in, jnp.zeros_like(x_in))
    bc_live = jnp.where(is_live[:, None], bc_in, jnp.zeros_like(bc_in))
    x_conv = conv_silu(x_live, conv_x_weight).astype(jnp.bfloat16)
    bc_conv = conv_silu(bc_live, conv_bc_weight).astype(jnp.bfloat16)
    step_size = jax.nn.softplus(dt_in.astype(jnp.float32) + dt_bias) * is_live.astype(jnp.float32)[:, None]
    log_decay = -a_rate * step_size
    blocks = length // SPAN
    x_blocks = x_conv.reshape(blocks, SPAN, HEADS, HEAD_DIM)
    b_blocks = bc_conv[:, :NSTATE].reshape(blocks, SPAN, NSTATE)
    c_blocks = bc_conv[:, NSTATE:].reshape(blocks, SPAN, NSTATE)
    step_blocks = step_size.reshape(blocks, SPAN, HEADS)
    decay_blocks = log_decay.reshape(blocks, SPAN, HEADS)

    def advance(state, inputs):
        input_block, b_block, c_block, step_block, decay_block = inputs
        cum_decay, y_intra, block_state, block_decay = span_terms(input_block[None], b_block[None], c_block[None], step_block[None], decay_block[None])
        from_state = jnp.exp(cum_decay[0])[:, :, None] * jnp.einsum('qn,hpn->qhp', c_block.astype(jnp.float32), state, precision=highest)
        y_out = y_intra[0] + from_state + d_skip[:, None] * input_block.astype(jnp.float32)
        return (block_decay[0][:, None, None] * state + block_state[0], y_out)
    start_state = jnp.zeros((HEADS, HEAD_DIM, NSTATE), jnp.float32)
    final_state, y_all = lax.scan(advance, start_state, (x_blocks, b_blocks, c_blocks, step_blocks, decay_blocks))
    y_flat = y_all.reshape(length, HEADS * HEAD_DIM)
    gated = y_flat * jax.nn.silu(z_in.astype(jnp.float32))
    mean_square = lax.optimization_barrier(jnp.mean(gated * gated, axis=1, keepdims=True))
    normed = (gated * lax.rsqrt(mean_square + stability_constant) * norm_gain).astype(jnp.bfloat16)
    mixed = jnp.dot(normed, out_weight, preferred_element_type=jnp.float32).astype(jnp.bfloat16)
    rim_rows = KCONV - 1
    return (mixed, final_state, x_live[length - rim_rows:], bc_live[length - rim_rows:])

def reference(x_proj, gate_proj, bc_proj, dt_proj, a_rate, dt_bias, d_skip, conv_x_weight, conv_bc_weight, norm_gain, out_weight, request_first_position, owner):
    length = TOK_DEV * N_SEQ
    rim_rows = KCONV - 1
    mixed_list = []
    state_list = []
    tail_x_list = []
    tail_bc_list = []
    for request in range(x_proj.shape[0]):
        mixed, final_state, tail_x, tail_bc = one_request(x_proj[request].reshape(length, -1), gate_proj[request].reshape(length, -1), bc_proj[request].reshape(length, -1), dt_proj[request].reshape(length, -1), request_first_position[request], a_rate, dt_bias, d_skip, conv_x_weight, conv_bc_weight, norm_gain, out_weight)
        inverse = jnp.argsort(owner[request]).astype(jnp.int32)
        slabs = final_state.reshape(HEADS, N_SEQ, -1)[:, inverse]
        state_list.append(jnp.transpose(slabs, (1, 0, 2)))
        x_slabs = tail_x.reshape(rim_rows, N_HEAD, N_SEQ, -1)[:, :, inverse]
        tail_x_list.append(jnp.transpose(x_slabs, (2, 0, 1, 3)).reshape(N_SEQ, rim_rows, -1))
        bc_slabs = tail_bc.reshape(rim_rows, N_SEQ, -1)[:, inverse]
        tail_bc_list.append(jnp.transpose(bc_slabs, (1, 0, 2)))
        mixed_list.append(mixed)
    return (jnp.stack(mixed_list), jnp.stack(state_list), jnp.stack(tail_x_list), jnp.stack(tail_bc_list))
```

```python
import functools

import jax
import jax.numpy as jnp
from jax import lax
from jax.experimental import pallas as pl
from jax.experimental.pallas import tpu as pltpu
from jax.sharding import PartitionSpec as P

HEAD_DIM = 64
NSTATE = 128
KCONV = 4
SPAN = 128
INNER = 8192


highest = lax.Precision.HIGHEST
stability_constant = 1e-05


def passed_along(value, axis, by):
    devices = lax.axis_size(axis)
    pairs = [(i, i + by) for i in range(devices) if 0 <= i + by < devices]
    return lax.ppermute(value, axis, pairs)


def prefix(value, axis, combine, identity, reverse):
    devices, place = (lax.axis_size(axis), lax.axis_index(axis))
    everything = jax.tree.map(lambda part: lax.all_gather(part, axis), value)
    start = jax.tree.map(
        lambda part, zero: jnp.broadcast_to(jnp.asarray(zero, part.dtype), part.shape),
        value,
        identity,
    )

    def lap(k, before):
        at = devices - 1 - k if reverse else k
        reached = at > place if reverse else at < place
        new = combine(before, jax.tree.map(lambda part: part[at], everything))
        return jax.tree.map(lambda a, b: jnp.where(reached, a, b), new, before)

    return lax.fori_loop(0, devices, lap, start)


def broadcast(block, axis, source):
    block = jnp.where(lax.axis_index(axis) == source, block, jnp.zeros_like(block))
    return lax.psum(block, axis)


def span_terms(x_conv, b_rows, c_rows, step_size, log_decay):
    cum_decay = jnp.cumsum(log_decay, axis=1)
    scores = jnp.einsum("kqn,ktn->kqt", c_rows, b_rows, preferred_element_type=jnp.float32)
    cum_heads = jnp.swapaxes(cum_decay, 1, 2)
    step_heads = jnp.swapaxes(step_size, 1, 2)
    block_len = cum_decay.shape[1]
    causal = jnp.arange(block_len)[:, None] >= jnp.arange(block_len)[None, :]
    decay_gap = cum_heads[:, :, :, None] - cum_heads[:, :, None, :]
    seg_decay = jnp.exp(jnp.where(causal, decay_gap, -jnp.inf))
    weights = (scores[:, None] * seg_decay * step_heads[:, :, None, :]).astype(jnp.bfloat16)
    y_intra = jnp.einsum("khqt,kthp->kqhp", weights, x_conv, preferred_element_type=jnp.float32)
    remaining_length = jnp.exp(cum_decay[:, -1:, :] - cum_decay)
    scaled = ((remaining_length * step_size)[..., None] * x_conv.astype(jnp.float32)).astype(
        jnp.bfloat16
    )
    states = jnp.einsum("kthp,ktn->khpn", scaled, b_rows, preferred_element_type=jnp.float32)
    return (cum_decay, y_intra, states, jnp.exp(cum_decay[:, -1, :]))


def conv_silu(preceding_tokens, current, weight):
    extended = jnp.concatenate([preceding_tokens, current], axis=0)
    length = current.shape[0]
    accum = jnp.zeros(current.shape, jnp.float32)
    for offset in range(weight.shape[0]):
        accum = accum + weight[offset] * extended[offset : offset + length].astype(jnp.float32)
    return jax.nn.silu(accum)


def link(preceding_tokens, later):
    return (
        preceding_tokens[0] * later[0],
        later[0][:, None, None] * preceding_tokens[1] + later[1],
    )


def multiply(preceding_tokens, later):
    return preceding_tokens * later


def add_rows(source, piece):
    return jnp.dot(source, piece, preferred_element_type=jnp.float32)


def take_slab(values, slab_index, seq_count):
    grouped = values.reshape(values.shape[0], seq_count, -1)
    return lax.dynamic_index_in_dim(grouped, slab_index, axis=1, keepdims=False)


def local(
    x_proj,
    gate_proj,
    bc_proj,
    dt_proj,
    a_rate,
    dt_bias,
    d_skip,
    conv_x_weight,
    conv_bc_weight,
    norm_gain,
    out_weight,
    request_first_position,
    owner,
):
    x_all, z_all, bc_all, dt_all = (
        lax.all_to_all(x_proj, "seq", split_axis=1, concat_axis=2, tiled=True),
        lax.all_to_all(gate_proj, "seq", split_axis=1, concat_axis=2, tiled=True),
        lax.all_to_all(bc_proj, "seq", split_axis=1, concat_axis=2, tiled=True),
        lax.all_to_all(dt_proj, "seq", split_axis=1, concat_axis=2, tiled=True),
    )
    tokens_here = x_all.shape[2] * x_all.shape[3]
    x_local = x_all.reshape(tokens_here, x_all.shape[4])
    z_local = z_all.reshape(tokens_here, z_all.shape[4])
    bc_local = bc_all.reshape(tokens_here, bc_all.shape[4])
    dt_local = dt_all.reshape(tokens_here, dt_all.shape[4])
    heads = dt_local.shape[1]
    seq_index = lax.axis_index("seq")
    seq_count = lax.axis_size("seq")
    positions = seq_index * tokens_here + jnp.arange(tokens_here, dtype=jnp.int32)
    is_live = positions >= request_first_position[0]
    x_live = jnp.where(is_live[:, None], x_local, jnp.zeros_like(x_local))
    bc_live = jnp.where(is_live[:, None], bc_local, jnp.zeros_like(bc_local))
    rim_rows = KCONV - 1
    tail_x = x_live[tokens_here - rim_rows :]
    tail_bc = bc_live[tokens_here - rim_rows :]
    before_x, before_bc = passed_along((tail_x, tail_bc), "seq", 1)
    x_conv = conv_silu(before_x, x_live, conv_x_weight).astype(jnp.bfloat16)
    bc_conv = conv_silu(before_bc, bc_live, conv_bc_weight).astype(jnp.bfloat16)
    step_size = (
        jax.nn.softplus(dt_local.astype(jnp.float32) + dt_bias)
        * is_live.astype(jnp.float32)[:, None]
    )
    log_decay = -a_rate * step_size
    blocks = tokens_here // SPAN
    x_blocks = x_conv.reshape(blocks, SPAN, heads, HEAD_DIM)
    b_blocks = bc_conv[:, :NSTATE].reshape(blocks, SPAN, NSTATE)
    c_blocks = bc_conv[:, NSTATE:].reshape(blocks, SPAN, NSTATE)
    cum_decay, y_intra, states, decays = span_terms(
        x_blocks,
        b_blocks,
        c_blocks,
        step_size.reshape(blocks, SPAN, heads),
        log_decay.reshape(blocks, SPAN, heads),
    )

    def advance(carry, inputs):
        factor, contrib = inputs
        return (factor[:, None, None] * carry + contrib, carry)

    zero_state = jnp.zeros((heads, HEAD_DIM, NSTATE), jnp.float32)
    local_final, local_enter = lax.scan(advance, zero_state, (decays, states))
    dev_decay = jnp.prod(decays, axis=0)
    ones_heads = jnp.ones((heads,), jnp.float32)
    enter_decay, enter_state = prefix(
        (dev_decay, local_final), "seq", link, (ones_heads, zero_state), False
    )
    c_wide = c_blocks.astype(jnp.float32)
    before_block = jnp.concatenate([ones_heads[None], jnp.cumprod(decays, axis=0)[:-1]], axis=0)
    entering = local_enter + before_block[:, :, None, None] * enter_state[None]
    y_state = jnp.exp(cum_decay)[..., None] * jnp.einsum(
        "kqn,khpn->kqhp", c_wide, entering, precision=highest
    )
    y_total = y_intra + y_state + d_skip[:, None] * x_blocks.astype(jnp.float32)
    y_flat = y_total.reshape(tokens_here, heads * HEAD_DIM)
    gated = y_flat * jax.nn.silu(z_local.astype(jnp.float32))
    square_sums = lax.psum(jnp.sum(gated * gated, axis=1), "head")
    normed = (
        gated * lax.rsqrt(square_sums[:, None] / INNER + stability_constant) * norm_gain
    ).astype(jnp.bfloat16)
    last_index = seq_count - 1
    after_decay = prefix(dev_decay, "seq", multiply, ones_heads, True)
    final_state = lax.psum(after_decay[:, None, None] * local_final, "seq")
    keep_x, keep_bc = (broadcast(tail_x, "seq", last_index), broadcast(tail_bc, "seq", last_index))
    slab_index = jnp.sum(
        jnp.where(owner[0] == seq_index, jnp.arange(seq_count, dtype=jnp.int32), 0)
    )
    ssm_state = take_slab(final_state.reshape(heads, -1), slab_index, seq_count)[None, None]
    conv_x_state = take_slab(keep_x, slab_index, seq_count)[None, None]
    conv_bc_state = take_slab(keep_bc, slab_index, seq_count)[None, None]
    features = lax.all_gather(normed, "head", axis=1, tiled=True)
    out_cols = out_weight.shape[1]
    mixed_sum = add_rows(features, lax.all_gather(out_weight, ("seq", "rep"), axis=0, tiled=True))
    mixed = mixed_sum.astype(jnp.bfloat16).reshape(1, tokens_here, out_cols)
    return (mixed, ssm_state, conv_x_state, conv_bc_state)


MESH = pl.DeviceIdType.MESH
LANES = 128
PAD = 8
F32 = jnp.float32
BF16 = jnp.bfloat16
NT = (((1,), (1,)), ((), ()))
TN = (((0,), (0,)), ((), ()))


def split3(value):
    hi = value.astype(BF16)
    rest = value - hi.astype(F32)
    mid = rest.astype(BF16)
    return hi, mid, (rest - mid.astype(F32)).astype(BF16)


def pick(parts, chosen):
    return sum(jnp.dot(parts[k], chosen, preferred_element_type=F32) for k in range(3))


def silu(value):
    return value * (1.0 / (1.0 + jnp.exp(-value)))


def fused_kernel(
    sizes,
    start_ref, owner_ref, x_ref, z_ref, bc_ref, dt_ref, rate_ref, bias_ref, skip_ref,
    cw_ref, cbw_ref, gain_ref, w_ref,
    mixed_ref, ssm_ref, tailx_ref, tailbc_ref,
    xs, zs, bcs, dts, xpad, bpad, b_scr, c_scr, cum3, step3, rows_t, scores, y_scr, g_scr,
    fin, fsnd, frecv, tails, wfull, psnd, precv, pown, qsnd, qrecv, ssnd, srecv,
    sx, rx, sz, rz, sb, rb, sd, rd, sw, rw, swf, rwf, st, rt, sf, rf, sp, rp, sq, rq, ss, rs,
):
    n_grp, n, n_head, n_rep = (sizes[a] for a in ("grp", "seq", "head", "rep"))
    me, head = lax.axis_index("seq"), lax.axis_index("head")
    grp, rep = lax.axis_index("grp"), lax.axis_index("rep")
    nb, _, sub, width = xs.shape
    length = nb * n * sub
    blocks = length // SPAN
    heads = dt_ref.shape[2]
    own_heads = heads // n
    out_cols = w_ref.shape[1]

    def exchange(src_of, dst_of, send, recv):
        copies = []
        for o in range(1, n):
            to = lax.rem(me + o, n)
            copies.append(pltpu.make_async_remote_copy(
                src_ref=src_of(to), dst_ref=dst_of, send_sem=send.at[o], recv_sem=recv.at[o],
                device_id={"seq": to}, device_id_type=MESH))
        own = pltpu.make_async_copy(src_of(me), dst_of, recv.at[0])
        for copy in copies:
            copy.start()
        own.start()
        return copies + [own]

    def cols(j):
        return pl.ds(pl.multiple_of(j * width, LANES), width)

    bc_copies = exchange(lambda j: bc_ref, bcs.at[:, me], sb, rb)
    dt_copies = exchange(lambda j: dt_ref, dts.at[:, me], sd, rd)
    x_copies = exchange(lambda j: x_ref.at[:, :, cols(j)], xs.at[:, me], sx, rx)
    z_copies = exchange(lambda j: z_ref.at[:, :, cols(j)], zs.at[:, me], sz, rz)

    w_rows = w_ref.shape[0] // n_grp
    part = me * n_rep + rep
    to_seq, to_head, to_rep = lax.rem(part, n), part // n, head
    w_self = (to_seq == me) & (to_head == head) & (to_rep == rep)

    def w_piece(g, c):
        return wfull.at[pl.ds(pl.multiple_of(g * w_rows, 16), w_rows),
                        pl.ds(pl.multiple_of(c * out_cols, LANES), out_cols)]

    w_src = w_ref.at[pl.ds(pl.multiple_of(grp * w_rows, 16), w_rows), :]
    w_copy = pltpu.make_async_remote_copy(
        src_ref=w_src, dst_ref=w_piece(grp, head), send_sem=sw, recv_sem=rw,
        device_id={"seq": to_seq, "head": to_head, "rep": to_rep}, device_id_type=MESH)

    @pl.when(w_self)
    def _():
        pltpu.make_async_copy(w_src, w_piece(grp, head), rw).start()

    @pl.when(jnp.logical_not(w_self))
    def _():
        w_copy.start()

    begin = start_ref[0]
    live = lax.broadcasted_iota(jnp.int32, (length, LANES), 0) >= begin
    row_id = lax.broadcasted_iota(jnp.int32, (SPAN, SPAN), 0)
    col_id = lax.broadcasted_iota(jnp.int32, (SPAN, SPAN), 1)
    causal = row_id >= col_id
    head_row = lax.broadcasted_iota(jnp.int32, (heads, LANES), 0)
    lane_head = lax.broadcasted_iota(jnp.int32, (heads, LANES), 1) // HEAD_DIM
    per_chunk = LANES // HEAD_DIM

    for copy in bc_copies + dt_copies:
        copy.wait()

    bpad[0:PAD, :] = jnp.zeros((PAD, bpad.shape[1]), F32)
    xpad[0:PAD, :] = jnp.zeros((PAD, LANES), F32)
    for half, target in ((0, b_scr), (1, c_scr)):
        at = pl.ds(half * NSTATE, NSTATE)
        bv = bcs[:, :, :, at].reshape(length, NSTATE).astype(F32)
        bpad[PAD:, at] = jnp.where(live, bv, 0.0)
        acc = jnp.zeros((length, NSTATE), F32)
        for k in range(KCONV):
            acc = acc + cbw_ref[k : k + 1, at] * bpad[pl.ds(PAD - KCONV + 1 + k, length), at]
        target[...] = silu(acc).astype(BF16)

    d = dts[...].reshape(length, heads).astype(F32) + bias_ref[...]
    step = jnp.maximum(d, 0.0) + jnp.log1p(jnp.exp(-jnp.abs(d)))
    step = jnp.where(live[:, :heads], step, 0.0)
    decay = -rate_ref[...] * step
    lower = causal.astype(F32)
    eye = (lax.broadcasted_iota(jnp.int32, (heads, heads), 0)
           == lax.broadcasted_iota(jnp.int32, (heads, heads), 1)).astype(F32)
    for c in range(blocks):
        r = slice(c * SPAN, (c + 1) * SPAN)
        cum = jnp.dot(lower, decay[r], precision=highest, preferred_element_type=F32)
        for k, (a, b) in enumerate(zip(split3(cum), split3(step[r]))):
            cum3[k, r, :] = a
            step3[k, r, :] = b
        rows_t[0, c] = lax.dot_general(eye, cum, NT, precision=highest, preferred_element_type=F32)
        rows_t[1, c] = lax.dot_general(eye, step[r], NT, precision=highest, preferred_element_type=F32)
        raw = lax.dot_general(c_scr[r, :], b_scr[r, :], NT, preferred_element_type=F32)
        scores[c] = jnp.where(causal, raw, 0.0)

    for copy in x_copies:
        copy.wait()
    tail_src = xs.at[nb - 1, n - 1, sub - 16 : sub, :]
    t_copies = exchange(lambda j: tail_src, tails.at[me], st, rt)

    left = lax.broadcasted_iota(jnp.int32, (SPAN, LANES), 1) < HEAD_DIM

    @pl.loop(0, width // LANES)
    def _(i):
        lanes = pl.ds(pl.multiple_of(i * LANES, LANES), LANES)
        wide = pl.ds(pl.multiple_of(me * width + i * LANES, LANES), LANES)
        xv = xs[:, :, :, lanes].reshape(length, LANES).astype(F32)
        xpad[PAD:, :] = jnp.where(live, xv, 0.0)
        acc = jnp.zeros((length, LANES), F32)
        for k in range(KCONV):
            acc = acc + cw_ref[k : k + 1, wide] * xpad[pl.ds(PAD - KCONV + 1 + k, length), :]
        xc = silu(acc).astype(BF16)
        first = me * own_heads + i * per_chunk
        chosen_f = (head_row == first + lane_head).astype(F32)
        chosen = chosen_f.astype(BF16)
        cum_l = pick(cum3, chosen)
        step_l = pick(step3, chosen)
        skip = jnp.dot(jnp.broadcast_to(skip_ref[...], (8, heads)), chosen_f, precision=highest,
                       preferred_element_type=F32)[0:1]
        state = jnp.zeros((NSTATE, LANES), F32)
        for c in range(blocks):
            r = slice(c * SPAN, (c + 1) * SPAN)
            cl, sl, xb = cum_l[r], step_l[r], xc[r]
            y = skip * xb.astype(F32)
            for k in range(per_chunk):
                cum_q = jnp.broadcast_to(cl[:, k * HEAD_DIM : k * HEAD_DIM + 1], (SPAN, SPAN))
                cum_t = rows_t[0, c, pl.ds(first + k, 1), :]
                step_t = rows_t[1, c, pl.ds(first + k, 1), :]
                mix = (scores[c] * jnp.exp(jnp.minimum(cum_q - cum_t, 0.0)) * step_t).astype(BF16)
                xk = jnp.where(left if k == 0 else jnp.logical_not(left), xb.astype(F32), 0.0).astype(BF16)
                y = y + jnp.dot(mix, xk, preferred_element_type=F32)
            if c:
                y = y + jnp.exp(cl) * jnp.dot(c_scr[r, :], state.astype(BF16), preferred_element_type=F32)
            y_scr[r, lanes] = y
            last = cl[SPAN - 1 : SPAN, :]
            scaled = (jnp.exp(last - cl) * sl * xb.astype(F32)).astype(BF16)
            state = jnp.exp(last) * state + lax.dot_general(
                b_scr[r, :], scaled, TN, preferred_element_type=F32)
        fin[pl.ds(i * per_chunk, per_chunk)] = state.T.reshape(per_chunk, n, HEAD_DIM // n, NSTATE)

    def slab_of(s):
        return jnp.minimum(sum(jnp.where(owner_ref[j] == s, j, 0) for j in range(n)), n - 1)

    f_copies = []
    for o in range(1, n):
        to = lax.rem(me + o, n)
        fsnd[o] = fin[:, slab_of(to)]
        f_copies.append(pltpu.make_async_remote_copy(
            src_ref=fsnd.at[o], dst_ref=frecv.at[me], send_sem=sf.at[o], recv_sem=rf.at[o],
            device_id={"seq": to}, device_id_type=MESH))

    for copy in z_copies:
        copy.wait()

    def gate_chunk(i, total):
        lanes = pl.ds(pl.multiple_of(i * LANES, LANES), LANES)
        wide = pl.ds(pl.multiple_of(me * width + i * LANES, LANES), LANES)
        zv = zs[:, :, :, lanes].reshape(length, LANES).astype(F32)
        gated = y_scr[:, lanes] * silu(zv)
        g_scr[:, lanes] = (gated * gain_ref[:, wide]).astype(BF16)
        return total + gated * gated

    squares = lax.fori_loop(0, width // LANES, gate_chunk, jnp.zeros((length, LANES), F32))
    for c in range(blocks):
        r = slice(c * SPAN, (c + 1) * SPAN)
        total = jnp.broadcast_to(jnp.sum(squares[r], axis=1, keepdims=True), (SPAN, LANES))
        ssnd[c] = total.T[0:8, :]

    @pl.when(w_self)
    def _():
        pltpu.make_async_copy(w_src, w_piece(grp, head), rw).wait()

    @pl.when(jnp.logical_not(w_self))
    def _():
        w_copy.wait()

    wf_copies = []
    for og in range(n_grp):
        for orr in range(n_rep):
            if og or orr:
                slot = og * n_rep + orr
                wf_copies.append(pltpu.make_async_remote_copy(
                    src_ref=w_piece(grp, rep), dst_ref=w_piece(grp, rep),
                    send_sem=swf.at[slot], recv_sem=rwf.at[slot],
                    device_id={"grp": lax.rem(grp + og, n_grp), "rep": lax.rem(rep + orr, n_rep)},
                    device_id_type=MESH))
    for copy in wf_copies:
        copy.start()

    s_copies = []
    for oh in range(n_head):
        for o in range(n):
            if oh or o:
                to = lax.rem(me + o, n)
                slot = oh * n + o
                s_copies.append(pltpu.make_async_remote_copy(
                    src_ref=ssnd.at[to], dst_ref=srecv.at[slot], send_sem=ss.at[slot],
                    recv_sem=rs.at[slot],
                    device_id={"seq": to, "head": lax.rem(head + oh, n_head)}, device_id_type=MESH))
    for copy in s_copies + f_copies:
        copy.start()
    for copy in wf_copies:
        copy.wait()

    tile = 256 if out_cols % 256 == 0 else LANES

    def product(h, put):
        @pl.loop(0, out_cols // tile)
        def _(i):
            at = pl.ds(pl.multiple_of(h * out_cols + i * tile, LANES), tile)
            out = jnp.dot(g_scr[...], wfull[:, at], preferred_element_type=F32)
            put(pl.ds(pl.multiple_of(i * tile, LANES), tile), out.reshape(blocks, SPAN, tile))

    p_copies = {}
    for oh in range(1, n_head):
        to_h = lax.rem(head + oh, n_head)

        def put(at, out, oh=oh):
            psnd[oh - 1, :, :, at] = out.astype(BF16)

        product(to_h, put)
        for o in [*range(1, n), 0]:
            block = lax.rem(me + o, n)
            p_copies[oh, o] = pltpu.make_async_remote_copy(
                src_ref=psnd.at[oh - 1, block], dst_ref=precv.at[oh - 1, block],
                send_sem=sp.at[oh - 1, o], recv_sem=rp.at[oh - 1, o],
                device_id={"head": to_h}, device_id_type=MESH)
            p_copies[oh, o].start()

    def put_own(at, out):
        pown[:, :, at] = out

    product(head, put_own)

    q_copies = []
    for o in [*range(1, n), 0]:
        block = lax.rem(me + o, n)
        whole = pown[block]
        for oh in range(1, n_head):
            p_copies[oh, o].wait()
            whole = whole + precv[oh - 1, block].astype(F32)
        if o:
            qsnd[o] = whole.astype(BF16)
            q_copies.append(pltpu.make_async_remote_copy(
                src_ref=qsnd.at[o], dst_ref=qrecv.at[o], send_sem=sq.at[o], recv_sem=rq.at[o],
                device_id={"seq": block}, device_id_type=MESH))
            q_copies[-1].start()
        else:
            pown[block] = whole

    for copy in s_copies + t_copies:
        copy.wait()
    total = ssnd[me]
    for slot in range(1, n * n_head):
        total = total + srecv[slot]
    scale_row = lax.rsqrt(total / INNER + stability_constant)
    scale = jnp.broadcast_to(scale_row[0:1], (SPAN, LANES)).T

    slab = slab_of(me)
    tail_live = length - 16 + lax.broadcasted_iota(jnp.int32, (16, width), 0) >= begin
    tailx_ref[...] = jnp.where(tail_live, tails[slab].astype(F32), 0.0).astype(BF16)
    state_cols = tailbc_ref.shape[1]
    wide_bc = bcs.shape[3]
    chosen = (lax.broadcasted_iota(jnp.int32, (wide_bc, state_cols), 0)
              == slab * state_cols + lax.broadcasted_iota(jnp.int32, (wide_bc, state_cols), 1)).astype(BF16)
    tailbc_ref[...] = jnp.dot(
        bpad[PAD + length - 16 : PAD + length, :].astype(BF16), chosen, preferred_element_type=F32).astype(BF16)

    for copy in f_copies:
        copy.wait()
    frecv[me] = fin[:, slab]
    ssm_ref[...] = frecv[...]

    for copy in q_copies:
        copy.wait()
    for at in range(0, out_cols, LANES):
        lanes = slice(at, at + LANES)
        whole = pown[me, :, lanes]
        for o in range(1, n):
            whole = whole + qrecv[o, :, lanes].astype(F32)
        mixed_ref[:, lanes] = (whole * scale).astype(BF16)


def fused(
    sizes, x_proj, gate_proj, bc_proj, dt_proj, a_rate, dt_bias, d_skip, conv_x_weight,
    conv_bc_weight, norm_gain, out_weight, request_first_position, owner,
):
    n_grp, n, n_head, n_rep = (sizes[a] for a in ("grp", "seq", "head", "rep"))
    nb, sub, channels = x_proj.shape[1], x_proj.shape[3], x_proj.shape[4]
    heads, bc_cols = dt_proj.shape[4], bc_proj.shape[4]
    length, width = nb * n * sub, channels // n
    blocks, own_heads, out_cols = length // SPAN, heads // n, out_weight.shape[1]
    piece = HEAD_DIM // n
    vmem = lambda shape, kind: pltpu.VMEM(shape, kind)
    dma = lambda *shape: pltpu.SemaphoreType.DMA(shape)
    hbm = pl.BlockSpec(memory_space=pl.ANY)
    here = pl.BlockSpec(memory_space=pltpu.VMEM)
    smem = pl.BlockSpec(memory_space=pltpu.SMEM)
    mixed, ssm, tail_x, tail_bc = pl.pallas_call(
        functools.partial(fused_kernel, sizes),
        out_shape=(
            jax.ShapeDtypeStruct((SPAN, out_cols), BF16),
            jax.ShapeDtypeStruct((n, own_heads, piece, NSTATE), F32),
            jax.ShapeDtypeStruct((16, width), BF16),
            jax.ShapeDtypeStruct((16, bc_cols // n), BF16),
        ),
        in_specs=[smem, smem, hbm, hbm, hbm, hbm] + [here] * 6 + [hbm],
        out_specs=(here,) * 4,
        scratch_shapes=[
            vmem((nb, n, sub, width), BF16),
            vmem((nb, n, sub, width), BF16),
            vmem((nb, n, sub, bc_cols), BF16),
            vmem((nb, n, sub, heads), BF16),
            vmem((length + PAD, LANES), F32),
            vmem((length + PAD, bc_cols), F32),
            vmem((length, NSTATE), BF16),
            vmem((length, NSTATE), BF16),
            vmem((3, length, heads), BF16),
            vmem((3, length, heads), BF16),
            vmem((2, blocks, heads, SPAN), F32),
            vmem((blocks, SPAN, SPAN), F32),
            vmem((length, width), F32),
            vmem((length, width), BF16),
            vmem((own_heads, n, piece, NSTATE), F32),
            vmem((n, own_heads, piece, NSTATE), F32),
            vmem((n, own_heads, piece, NSTATE), F32),
            vmem((n, 16, width), BF16),
            vmem((width, out_cols * n_head), BF16),
            vmem((n_head - 1, blocks, SPAN, out_cols), BF16),
            vmem((n_head - 1, blocks, SPAN, out_cols), BF16),
            vmem((blocks, SPAN, out_cols), F32),
            vmem((n, SPAN, out_cols), BF16),
            vmem((n, SPAN, out_cols), BF16),
            vmem((blocks, 8, LANES), F32),
            vmem((n * n_head, 8, LANES), F32),
            dma(n), dma(n), dma(n), dma(n), dma(n), dma(n), dma(n), dma(n),
            pltpu.SemaphoreType.DMA, pltpu.SemaphoreType.DMA,
            dma(n_grp * n_rep), dma(n_grp * n_rep),
            dma(n), dma(n), dma(n), dma(n),
            dma(n_head - 1, n), dma(n_head - 1, n),
            dma(n), dma(n), dma(n * n_head), dma(n * n_head),
        ],
        compiler_params=pltpu.CompilerParams(
            has_side_effects=True, vmem_limit_bytes=56 * 1024 * 1024
        ),
    )(
        request_first_position,
        owner.reshape(n),
        x_proj.reshape(nb, sub, channels),
        gate_proj.reshape(nb, sub, channels),
        bc_proj.reshape(nb, sub, bc_cols),
        dt_proj.reshape(nb, sub, heads),
        a_rate[None],
        dt_bias[None],
        d_skip[None],
        conv_x_weight,
        conv_bc_weight,
        norm_gain[None],
        out_weight,
    )
    rim = KCONV - 1
    return (
        mixed[None],
        ssm.reshape(1, 1, heads, piece * NSTATE),
        tail_x[16 - rim :][None, None],
        tail_bc[16 - rim :][None, None],
    )


def either(sizes, x_proj, *rest):
    n, n_head, n_rep = sizes["seq"], sizes["head"], sizes["rep"]
    nb, sub, channels = x_proj.shape[1], x_proj.shape[3], x_proj.shape[4]
    fits = (
        nb * sub == SPAN
        and nb == n
        and sub % 16 == 0
        and n_head == n_rep
        and channels % (n * LANES) == 0
        and rest[9].shape[0] * n == channels
    )
    return fused(sizes, x_proj, *rest) if fits else local(x_proj, *rest)


def solution(mesh):
    return jax.shard_map(
        functools.partial(either, dict(mesh.shape)),
        mesh=mesh,
        in_specs=(
            P(("grp", "rep"), None, "seq", None, "head"),
            P(("grp", "rep"), None, "seq", None, "head"),
            P(("grp", "rep"), None, "seq", None, None),
            P(("grp", "rep"), None, "seq", None, "head"),
            P("head"),
            P("head"),
            P("head"),
            P(None, "head"),
            P(),
            P("head"),
            P(("seq", "rep"), "head"),
            P(("grp", "rep")),
            P(("grp", "rep"), None),
        ),
        out_specs=(
            P(("grp", "rep"), "seq", "head"),
            P(("grp", "rep"), "seq", "head", None),
            P(("grp", "rep"), "seq", None, "head"),
            P(("grp", "rep"), "seq", None, None),
        ),
        check_vma=False,
    )
```

```python
import functools

import jax
import jax.numpy as jnp
from jax import lax
from jax.experimental import pallas as pl
from jax.experimental.pallas import tpu as pltpu
from jax.sharding import PartitionSpec as P

HEAD_DIM = 64
NSTATE = 128
KCONV = 4
SPAN = 128
INNER = 8192


highest = lax.Precision.HIGHEST
stability_constant = 1e-05


def passed_along(value, axis, by):
    devices = lax.axis_size(axis)
    pairs = [(i, i + by) for i in range(devices) if 0 <= i + by < devices]
    return lax.ppermute(value, axis, pairs)


def prefix(value, axis, combine, identity, reverse):
    devices, place = (lax.axis_size(axis), lax.axis_index(axis))
    everything = jax.tree.map(lambda part: lax.all_gather(part, axis), value)
    start = jax.tree.map(
        lambda part, zero: jnp.broadcast_to(jnp.asarray(zero, part.dtype), part.shape),
        value,
        identity,
    )

    def lap(k, before):
        at = devices - 1 - k if reverse else k
        reached = at > place if reverse else at < place
        new = combine(before, jax.tree.map(lambda part: part[at], everything))
        return jax.tree.map(lambda a, b: jnp.where(reached, a, b), new, before)

    return lax.fori_loop(0, devices, lap, start)


def broadcast(block, axis, source):
    block = jnp.where(lax.axis_index(axis) == source, block, jnp.zeros_like(block))
    return lax.psum(block, axis)


def span_terms(x_conv, b_rows, c_rows, step_size, log_decay):
    cum_decay = jnp.cumsum(log_decay, axis=1)
    scores = jnp.einsum("kqn,ktn->kqt", c_rows, b_rows, preferred_element_type=jnp.float32)
    cum_heads = jnp.swapaxes(cum_decay, 1, 2)
    step_heads = jnp.swapaxes(step_size, 1, 2)
    block_len = cum_decay.shape[1]
    causal = jnp.arange(block_len)[:, None] >= jnp.arange(block_len)[None, :]
    decay_gap = cum_heads[:, :, :, None] - cum_heads[:, :, None, :]
    seg_decay = jnp.exp(jnp.where(causal, decay_gap, -jnp.inf))
    weights = (scores[:, None] * seg_decay * step_heads[:, :, None, :]).astype(jnp.bfloat16)
    y_intra = jnp.einsum("khqt,kthp->kqhp", weights, x_conv, preferred_element_type=jnp.float32)
    remaining_length = jnp.exp(cum_decay[:, -1:, :] - cum_decay)
    scaled = ((remaining_length * step_size)[..., None] * x_conv.astype(jnp.float32)).astype(
        jnp.bfloat16
    )
    states = jnp.einsum("kthp,ktn->khpn", scaled, b_rows, preferred_element_type=jnp.float32)
    return (cum_decay, y_intra, states, jnp.exp(cum_decay[:, -1, :]))


def conv_silu(preceding_tokens, current, weight):
    extended = jnp.concatenate([preceding_tokens, current], axis=0)
    length = current.shape[0]
    accum = jnp.zeros(current.shape, jnp.float32)
    for offset in range(weight.shape[0]):
        accum = accum + weight[offset] * extended[offset : offset + length].astype(jnp.float32)
    return jax.nn.silu(accum)


def link(preceding_tokens, later):
    return (
        preceding_tokens[0] * later[0],
        later[0][:, None, None] * preceding_tokens[1] + later[1],
    )


def multiply(preceding_tokens, later):
    return preceding_tokens * later


def add_rows(source, piece):
    return jnp.dot(source, piece, preferred_element_type=jnp.float32)


def take_slab(values, slab_index, seq_count):
    grouped = values.reshape(values.shape[0], seq_count, -1)
    return lax.dynamic_index_in_dim(grouped, slab_index, axis=1, keepdims=False)


def local(
    x_proj,
    gate_proj,
    bc_proj,
    dt_proj,
    a_rate,
    dt_bias,
    d_skip,
    conv_x_weight,
    conv_bc_weight,
    norm_gain,
    out_weight,
    request_first_position,
    owner,
):
    x_all, z_all, bc_all, dt_all = (
        lax.all_to_all(x_proj, "seq", split_axis=1, concat_axis=2, tiled=True),
        lax.all_to_all(gate_proj, "seq", split_axis=1, concat_axis=2, tiled=True),
        lax.all_to_all(bc_proj, "seq", split_axis=1, concat_axis=2, tiled=True),
        lax.all_to_all(dt_proj, "seq", split_axis=1, concat_axis=2, tiled=True),
    )
    tokens_here = x_all.shape[2] * x_all.shape[3]
    x_local = x_all.reshape(tokens_here, x_all.shape[4])
    z_local = z_all.reshape(tokens_here, z_all.shape[4])
    bc_local = bc_all.reshape(tokens_here, bc_all.shape[4])
    dt_local = dt_all.reshape(tokens_here, dt_all.shape[4])
    heads = dt_local.shape[1]
    seq_index = lax.axis_index("seq")
    seq_count = lax.axis_size("seq")
    positions = seq_index * tokens_here + jnp.arange(tokens_here, dtype=jnp.int32)
    is_live = positions >= request_first_position[0]
    x_live = jnp.where(is_live[:, None], x_local, jnp.zeros_like(x_local))
    bc_live = jnp.where(is_live[:, None], bc_local, jnp.zeros_like(bc_local))
    rim_rows = KCONV - 1
    tail_x = x_live[tokens_here - rim_rows :]
    tail_bc = bc_live[tokens_here - rim_rows :]
    before_x, before_bc = passed_along((tail_x, tail_bc), "seq", 1)
    x_conv = conv_silu(before_x, x_live, conv_x_weight).astype(jnp.bfloat16)
    bc_conv = conv_silu(before_bc, bc_live, conv_bc_weight).astype(jnp.bfloat16)
    step_size = (
        jax.nn.softplus(dt_local.astype(jnp.float32) + dt_bias)
        * is_live.astype(jnp.float32)[:, None]
    )
    log_decay = -a_rate * step_size
    blocks = tokens_here // SPAN
    x_blocks = x_conv.reshape(blocks, SPAN, heads, HEAD_DIM)
    b_blocks = bc_conv[:, :NSTATE].reshape(blocks, SPAN, NSTATE)
    c_blocks = bc_conv[:, NSTATE:].reshape(blocks, SPAN, NSTATE)
    cum_decay, y_intra, states, decays = span_terms(
        x_blocks,
        b_blocks,
        c_blocks,
        step_size.reshape(blocks, SPAN, heads),
        log_decay.reshape(blocks, SPAN, heads),
    )

    def advance(carry, inputs):
        factor, contrib = inputs
        return (factor[:, None, None] * carry + contrib, carry)

    zero_state = jnp.zeros((heads, HEAD_DIM, NSTATE), jnp.float32)
    local_final, local_enter = lax.scan(advance, zero_state, (decays, states))
    dev_decay = jnp.prod(decays, axis=0)
    ones_heads = jnp.ones((heads,), jnp.float32)
    enter_decay, enter_state = prefix(
        (dev_decay, local_final), "seq", link, (ones_heads, zero_state), False
    )
    c_wide = c_blocks.astype(jnp.float32)
    before_block = jnp.concatenate([ones_heads[None], jnp.cumprod(decays, axis=0)[:-1]], axis=0)
    entering = local_enter + before_block[:, :, None, None] * enter_state[None]
    y_state = jnp.exp(cum_decay)[..., None] * jnp.einsum(
        "kqn,khpn->kqhp", c_wide, entering, precision=highest
    )
    y_total = y_intra + y_state + d_skip[:, None] * x_blocks.astype(jnp.float32)
    y_flat = y_total.reshape(tokens_here, heads * HEAD_DIM)
    gated = y_flat * jax.nn.silu(z_local.astype(jnp.float32))
    square_sums = lax.psum(jnp.sum(gated * gated, axis=1), "head")
    normed = (
        gated * lax.rsqrt(square_sums[:, None] / INNER + stability_constant) * norm_gain
    ).astype(jnp.bfloat16)
    last_index = seq_count - 1
    after_decay = prefix(dev_decay, "seq", multiply, ones_heads, True)
    final_state = lax.psum(after_decay[:, None, None] * local_final, "seq")
    keep_x, keep_bc = (broadcast(tail_x, "seq", last_index), broadcast(tail_bc, "seq", last_index))
    slab_index = jnp.sum(
        jnp.where(owner[0] == seq_index, jnp.arange(seq_count, dtype=jnp.int32), 0)
    )
    ssm_state = take_slab(final_state.reshape(heads, -1), slab_index, seq_count)[None, None]
    conv_x_state = take_slab(keep_x, slab_index, seq_count)[None, None]
    conv_bc_state = take_slab(keep_bc, slab_index, seq_count)[None, None]
    features = lax.all_gather(normed, "head", axis=1, tiled=True)
    out_cols = out_weight.shape[1]
    mixed_sum = add_rows(features, lax.all_gather(out_weight, ("seq", "rep"), axis=0, tiled=True))
    mixed = mixed_sum.astype(jnp.bfloat16).reshape(1, tokens_here, out_cols)
    return (mixed, ssm_state, conv_x_state, conv_bc_state)


MESH = pl.DeviceIdType.MESH
LANES = 128
PAD = 8
F32 = jnp.float32
BF16 = jnp.bfloat16
NT = (((1,), (1,)), ((), ()))
TN = (((0,), (0,)), ((), ()))


def split3(value):
    hi = value.astype(BF16)
    rest = value - hi.astype(F32)
    mid = rest.astype(BF16)
    return hi, mid, (rest - mid.astype(F32)).astype(BF16)


def pick(parts, chosen):
    return sum(jnp.dot(parts[k], chosen, preferred_element_type=F32) for k in range(3))


def silu(value):
    return value * (1.0 / (1.0 + jnp.exp(-value)))


def fused_kernel(
    sizes,
    start_ref, owner_ref, x_ref, z_ref, bc_ref, dt_ref, rate_ref, bias_ref, skip_ref,
    cw_ref, cbw_ref, gain_ref, w_ref,
    mixed_ref, ssm_ref, tailx_ref, tailbc_ref,
    xs, zs, bcs, dts, xpad, bpad, b_scr, c_scr, cum3, step3, rows_t, scores, y_scr, g_scr,
    fin, fsnd, frecv, tails, wfull, psnd, precv, pown, qsnd, qrecv, ssnd, srecv,
    sx, rx, sz, rz, sb, rb, sd, rd, sw, rw, swf, rwf, st, rt, sf, rf, sp, rp, sq, rq, ss, rs,
):
    n_grp, n, n_head, n_rep = (sizes[a] for a in ("grp", "seq", "head", "rep"))
    me, head = lax.axis_index("seq"), lax.axis_index("head")
    grp, rep = lax.axis_index("grp"), lax.axis_index("rep")
    nb, _, sub, width = xs.shape
    length = nb * n * sub
    blocks = length // SPAN
    heads = dt_ref.shape[2]
    own_heads = heads // n
    out_cols = w_ref.shape[1]

    def exchange(src_of, dst_of, send, recv):
        copies = []
        for o in range(1, n):
            to = lax.rem(me + o, n)
            copies.append(pltpu.make_async_remote_copy(
                src_ref=src_of(to), dst_ref=dst_of, send_sem=send.at[o], recv_sem=recv.at[o],
                device_id={"seq": to}, device_id_type=MESH))
        own = pltpu.make_async_copy(src_of(me), dst_of, recv.at[0])
        for copy in copies:
            copy.start()
        own.start()
        return copies + [own]

    def cols(j):
        return pl.ds(pl.multiple_of(j * width, LANES), width)

    bc_copies = exchange(lambda j: bc_ref, bcs.at[:, me], sb, rb)
    dt_copies = exchange(lambda j: dt_ref, dts.at[:, me], sd, rd)

    w_rows = w_ref.shape[0] // n_grp
    part = me * n_rep + rep
    to_seq, to_head, to_rep = lax.rem(part, n), part // n, head
    w_self = (to_seq == me) & (to_head == head) & (to_rep == rep)

    def w_piece(g, c):
        return wfull.at[pl.ds(pl.multiple_of(g * w_rows, 16), w_rows),
                        pl.ds(pl.multiple_of(c * out_cols, LANES), out_cols)]

    w_src = w_ref.at[pl.ds(pl.multiple_of(grp * w_rows, 16), w_rows), :]
    w_copy = pltpu.make_async_remote_copy(
        src_ref=w_src, dst_ref=w_piece(grp, head), send_sem=sw, recv_sem=rw,
        device_id={"seq": to_seq, "head": to_head, "rep": to_rep}, device_id_type=MESH)

    @pl.when(w_self)
    def _():
        pltpu.make_async_copy(w_src, w_piece(grp, head), rw).start()

    @pl.when(jnp.logical_not(w_self))
    def _():
        w_copy.start()

    x_copies = exchange(lambda j: x_ref.at[:, :, cols(j)], xs.at[:, me], sx, rx)
    z_copies = exchange(lambda j: z_ref.at[:, :, cols(j)], zs.at[:, me], sz, rz)

    begin = start_ref[0]
    live = lax.broadcasted_iota(jnp.int32, (length, LANES), 0) >= begin
    row_id = lax.broadcasted_iota(jnp.int32, (SPAN, SPAN), 0)
    col_id = lax.broadcasted_iota(jnp.int32, (SPAN, SPAN), 1)
    causal = row_id >= col_id
    head_row = lax.broadcasted_iota(jnp.int32, (heads, LANES), 0)
    lane_head = lax.broadcasted_iota(jnp.int32, (heads, LANES), 1) // HEAD_DIM
    per_chunk = LANES // HEAD_DIM

    for copy in bc_copies + dt_copies:
        copy.wait()

    bpad[0:PAD, :] = jnp.zeros((PAD, bpad.shape[1]), F32)
    xpad[0:PAD, :] = jnp.zeros((PAD, LANES), F32)
    for half, target in ((0, b_scr), (1, c_scr)):
        at = pl.ds(half * NSTATE, NSTATE)
        bv = bcs[:, :, :, at].reshape(length, NSTATE).astype(F32)
        bpad[PAD:, at] = jnp.where(live, bv, 0.0)
        acc = jnp.zeros((length, NSTATE), F32)
        for k in range(KCONV):
            acc = acc + cbw_ref[k : k + 1, at] * bpad[pl.ds(PAD - KCONV + 1 + k, length), at]
        target[...] = silu(acc).astype(BF16)

    d = dts[...].reshape(length, heads).astype(F32) + bias_ref[...]
    step = jnp.maximum(d, 0.0) + jnp.log1p(jnp.exp(-jnp.abs(d)))
    step = jnp.where(live[:, :heads], step, 0.0)
    decay = -rate_ref[...] * step
    lower = causal.astype(F32)
    eye = (lax.broadcasted_iota(jnp.int32, (heads, heads), 0)
           == lax.broadcasted_iota(jnp.int32, (heads, heads), 1)).astype(F32)
    for c in range(blocks):
        r = slice(c * SPAN, (c + 1) * SPAN)
        cum = jnp.dot(lower, decay[r], precision=highest, preferred_element_type=F32)
        for k, (a, b) in enumerate(zip(split3(cum), split3(step[r]))):
            cum3[k, r, :] = a
            step3[k, r, :] = b
        rows_t[0, c] = lax.dot_general(eye, cum, NT, precision=highest, preferred_element_type=F32)
        rows_t[1, c] = lax.dot_general(eye, step[r], NT, precision=highest, preferred_element_type=F32)
        raw = lax.dot_general(c_scr[r, :], b_scr[r, :], NT, preferred_element_type=F32)
        scores[c] = jnp.where(causal, raw, 0.0)

    @pl.when(w_self)
    def _():
        pltpu.make_async_copy(w_src, w_piece(grp, head), rw).wait()

    @pl.when(jnp.logical_not(w_self))
    def _():
        w_copy.wait()

    wf_copies = []
    for og in range(n_grp):
        for orr in range(n_rep):
            if og or orr:
                slot = og * n_rep + orr
                wf_copies.append(pltpu.make_async_remote_copy(
                    src_ref=w_piece(grp, rep), dst_ref=w_piece(grp, rep),
                    send_sem=swf.at[slot], recv_sem=rwf.at[slot],
                    device_id={"grp": lax.rem(grp + og, n_grp), "rep": lax.rem(rep + orr, n_rep)},
                    device_id_type=MESH))
    for copy in wf_copies:
        copy.start()

    for copy in x_copies:
        copy.wait()
    tail_src = xs.at[nb - 1, n - 1, sub - 16 : sub, :]
    t_copies = exchange(lambda j: tail_src, tails.at[me], st, rt)

    left = lax.broadcasted_iota(jnp.int32, (SPAN, LANES), 1) < HEAD_DIM

    @pl.loop(0, width // LANES)
    def _(i):
        lanes = pl.ds(pl.multiple_of(i * LANES, LANES), LANES)
        wide = pl.ds(pl.multiple_of(me * width + i * LANES, LANES), LANES)
        xv = xs[:, :, :, lanes].reshape(length, LANES).astype(F32)
        xpad[PAD:, :] = jnp.where(live, xv, 0.0)
        acc = jnp.zeros((length, LANES), F32)
        for k in range(KCONV):
            acc = acc + cw_ref[k : k + 1, wide] * xpad[pl.ds(PAD - KCONV + 1 + k, length), :]
        xc = silu(acc).astype(BF16)
        first = me * own_heads + i * per_chunk
        chosen_f = (head_row == first + lane_head).astype(F32)
        chosen = chosen_f.astype(BF16)
        cum_l = pick(cum3, chosen)
        step_l = pick(step3, chosen)
        skip = jnp.dot(jnp.broadcast_to(skip_ref[...], (8, heads)), chosen_f, precision=highest,
                       preferred_element_type=F32)[0:1]
        state = jnp.zeros((NSTATE, LANES), F32)
        for c in range(blocks):
            r = slice(c * SPAN, (c + 1) * SPAN)
            cl, sl, xb = cum_l[r], step_l[r], xc[r]
            y = skip * xb.astype(F32)
            for k in range(per_chunk):
                cum_q = jnp.broadcast_to(cl[:, k * HEAD_DIM : k * HEAD_DIM + 1], (SPAN, SPAN))
                cum_t = rows_t[0, c, pl.ds(first + k, 1), :]
                step_t = rows_t[1, c, pl.ds(first + k, 1), :]
                mix = (scores[c] * jnp.exp(jnp.minimum(cum_q - cum_t, 0.0)) * step_t).astype(BF16)
                xk = jnp.where(left if k == 0 else jnp.logical_not(left), xb.astype(F32), 0.0).astype(BF16)
                y = y + jnp.dot(mix, xk, preferred_element_type=F32)
            if c:
                y = y + jnp.exp(cl) * jnp.dot(c_scr[r, :], state.astype(BF16), preferred_element_type=F32)
            y_scr[r, lanes] = y
            last = cl[SPAN - 1 : SPAN, :]
            scaled = (jnp.exp(last - cl) * sl * xb.astype(F32)).astype(BF16)
            state = jnp.exp(last) * state + lax.dot_general(
                b_scr[r, :], scaled, TN, preferred_element_type=F32)
        turned = state.T
        piece = HEAD_DIM // n
        for k in range(per_chunk):
            for p in range(HEAD_DIM):
                fin[p // piece, p % piece, pl.ds(i * per_chunk + k, 1), :] = (
                    turned[k * HEAD_DIM + p : k * HEAD_DIM + p + 1, :])

    def slab_of(s):
        return jnp.minimum(sum(jnp.where(owner_ref[j] == s, j, 0) for j in range(n)), n - 1)

    f_copies = []
    for o in range(1, n):
        to = lax.rem(me + o, n)
        fsnd[o] = fin[slab_of(to)].astype(BF16)
        f_copies.append(pltpu.make_async_remote_copy(
            src_ref=fsnd.at[o], dst_ref=frecv.at[me], send_sem=sf.at[o], recv_sem=rf.at[o],
            device_id={"seq": to}, device_id_type=MESH))
        f_copies[-1].start()

    for copy in z_copies:
        copy.wait()

    def gate_chunk(i, total):
        lanes = pl.ds(pl.multiple_of(i * LANES, LANES), LANES)
        wide = pl.ds(pl.multiple_of(me * width + i * LANES, LANES), LANES)
        zv = zs[:, :, :, lanes].reshape(length, LANES).astype(F32)
        gated = y_scr[:, lanes] * silu(zv)
        g_scr[:, lanes] = (gated * gain_ref[:, wide]).astype(BF16)
        return total + gated * gated

    squares = lax.fori_loop(0, width // LANES, gate_chunk, jnp.zeros((length, LANES), F32))
    for c in range(blocks):
        r = slice(c * SPAN, (c + 1) * SPAN)
        total = jnp.broadcast_to(jnp.sum(squares[r], axis=1, keepdims=True), (SPAN, LANES))
        ssnd[c] = total.T[0:8, :]

    s_copies = []
    for oh in range(n_head):
        for o in range(n):
            if oh or o:
                to = lax.rem(me + o, n)
                slot = oh * n + o
                s_copies.append(pltpu.make_async_remote_copy(
                    src_ref=ssnd.at[to], dst_ref=srecv.at[slot], send_sem=ss.at[slot],
                    recv_sem=rs.at[slot],
                    device_id={"seq": to, "head": lax.rem(head + oh, n_head)}, device_id_type=MESH))
    for copy in s_copies:
        copy.start()
    for copy in wf_copies:
        copy.wait()

    tile = 256 if out_cols % 256 == 0 else LANES

    def product(h, put):
        @pl.loop(0, out_cols // tile)
        def _(i):
            at = pl.ds(pl.multiple_of(h * out_cols + i * tile, LANES), tile)
            out = jnp.dot(g_scr[...], wfull[:, at], preferred_element_type=F32)
            put(pl.ds(pl.multiple_of(i * tile, LANES), tile), out.reshape(blocks, SPAN, tile))

    p_copies = {}
    for oh in range(1, n_head):
        to_h = lax.rem(head + oh, n_head)

        def put(at, out, oh=oh):
            psnd[oh - 1, :, :, at] = out.astype(BF16)

        product(to_h, put)
        for o in [*range(1, n), 0]:
            block = lax.rem(me + o, n)
            p_copies[oh, o] = pltpu.make_async_remote_copy(
                src_ref=psnd.at[oh - 1, block], dst_ref=precv.at[oh - 1, block],
                send_sem=sp.at[oh - 1, o], recv_sem=rp.at[oh - 1, o],
                device_id={"head": to_h}, device_id_type=MESH)
            p_copies[oh, o].start()

    def put_own(at, out):
        pown[:, :, at] = out

    product(head, put_own)

    q_copies = []
    for o in [*range(1, n), 0]:
        block = lax.rem(me + o, n)
        whole = pown[block]
        for oh in range(1, n_head):
            p_copies[oh, o].wait()
            whole = whole + precv[oh - 1, block].astype(F32)
        if o:
            qsnd[o] = whole.astype(BF16)
            q_copies.append(pltpu.make_async_remote_copy(
                src_ref=qsnd.at[o], dst_ref=qrecv.at[o], send_sem=sq.at[o], recv_sem=rq.at[o],
                device_id={"seq": block}, device_id_type=MESH))
            q_copies[-1].start()
        else:
            pown[block] = whole

    for copy in s_copies + t_copies:
        copy.wait()
    total = ssnd[me]
    for slot in range(1, n * n_head):
        total = total + srecv[slot]
    scale_row = lax.rsqrt(total / INNER + stability_constant)
    scale = jnp.broadcast_to(scale_row[0:1], (SPAN, LANES)).T

    slab = slab_of(me)
    tail_live = length - 16 + lax.broadcasted_iota(jnp.int32, (16, width), 0) >= begin
    rim = KCONV - 1
    kept = jnp.where(tail_live, tails[slab].astype(F32), 0.0)
    tailx_ref[...] = kept[16 - rim :].astype(BF16)
    state_cols = tailbc_ref.shape[1]
    wide_bc = bcs.shape[3]
    chosen = (lax.broadcasted_iota(jnp.int32, (wide_bc, state_cols), 0)
              == slab * state_cols + lax.broadcasted_iota(jnp.int32, (wide_bc, state_cols), 1)).astype(BF16)
    kept = jnp.dot(
        bpad[PAD + length - 16 : PAD + length, :].astype(BF16), chosen, preferred_element_type=F32)
    tailbc_ref[...] = kept[16 - rim :].astype(BF16)

    for copy in f_copies:
        copy.wait()
    for o in range(n):
        source = lax.rem(me + n - o, n)
        for p in range(HEAD_DIM // n):
            value = frecv[source, p].astype(F32) if o else fin[slab, p]
            ssm_ref[source, :, p * NSTATE : (p + 1) * NSTATE] = value

    for copy in q_copies:
        copy.wait()
    for at in range(0, out_cols, LANES):
        lanes = slice(at, at + LANES)
        whole = pown[me, :, lanes]
        for o in range(1, n):
            whole = whole + qrecv[o, :, lanes].astype(F32)
        mixed_ref[:, lanes] = (whole * scale).astype(BF16)


def fused(
    sizes, x_proj, gate_proj, bc_proj, dt_proj, a_rate, dt_bias, d_skip, conv_x_weight,
    conv_bc_weight, norm_gain, out_weight, request_first_position, owner,
):
    n_grp, n, n_head, n_rep = (sizes[a] for a in ("grp", "seq", "head", "rep"))
    nb, sub, channels = x_proj.shape[1], x_proj.shape[3], x_proj.shape[4]
    heads, bc_cols = dt_proj.shape[4], bc_proj.shape[4]
    length, width = nb * n * sub, channels // n
    blocks, own_heads, out_cols = length // SPAN, heads // n, out_weight.shape[1]
    piece = HEAD_DIM // n
    vmem = lambda shape, kind: pltpu.VMEM(shape, kind)
    dma = lambda *shape: pltpu.SemaphoreType.DMA(shape)
    hbm = pl.BlockSpec(memory_space=pl.ANY)
    here = pl.BlockSpec(memory_space=pltpu.VMEM)
    smem = pl.BlockSpec(memory_space=pltpu.SMEM)
    mixed, ssm, tail_x, tail_bc = pl.pallas_call(
        functools.partial(fused_kernel, sizes),
        out_shape=(
            jax.ShapeDtypeStruct((SPAN, out_cols), BF16),
            jax.ShapeDtypeStruct((n, own_heads, piece * NSTATE), F32),
            jax.ShapeDtypeStruct((KCONV - 1, width), BF16),
            jax.ShapeDtypeStruct((KCONV - 1, bc_cols // n), BF16),
        ),
        in_specs=[smem, smem, hbm, hbm, hbm, hbm] + [here] * 6 + [hbm],
        out_specs=(here,) * 4,
        scratch_shapes=[
            vmem((nb, n, sub, width), BF16),
            vmem((nb, n, sub, width), BF16),
            vmem((nb, n, sub, bc_cols), BF16),
            vmem((nb, n, sub, heads), BF16),
            vmem((length + PAD, LANES), F32),
            vmem((length + PAD, bc_cols), F32),
            vmem((length, NSTATE), BF16),
            vmem((length, NSTATE), BF16),
            vmem((3, length, heads), BF16),
            vmem((3, length, heads), BF16),
            vmem((2, blocks, heads, SPAN), F32),
            vmem((blocks, SPAN, SPAN), F32),
            vmem((length, width), F32),
            vmem((length, width), BF16),
            vmem((n, piece, own_heads, NSTATE), F32),
            vmem((n, piece, own_heads, NSTATE), BF16),
            vmem((n, piece, own_heads, NSTATE), BF16),
            vmem((n, 16, width), BF16),
            vmem((width, out_cols * n_head), BF16),
            vmem((n_head - 1, blocks, SPAN, out_cols), BF16),
            vmem((n_head - 1, blocks, SPAN, out_cols), BF16),
            vmem((blocks, SPAN, out_cols), F32),
            vmem((n, SPAN, out_cols), BF16),
            vmem((n, SPAN, out_cols), BF16),
            vmem((blocks, 8, LANES), F32),
            vmem((n * n_head, 8, LANES), F32),
            dma(n), dma(n), dma(n), dma(n), dma(n), dma(n), dma(n), dma(n),
            pltpu.SemaphoreType.DMA, pltpu.SemaphoreType.DMA,
            dma(n_grp * n_rep), dma(n_grp * n_rep),
            dma(n), dma(n), dma(n), dma(n),
            dma(n_head - 1, n), dma(n_head - 1, n),
            dma(n), dma(n), dma(n * n_head), dma(n * n_head),
        ],
        compiler_params=pltpu.CompilerParams(
            has_side_effects=True, vmem_limit_bytes=56 * 1024 * 1024
        ),
    )(
        request_first_position,
        owner.reshape(n),
        x_proj.reshape(nb, sub, channels),
        gate_proj.reshape(nb, sub, channels),
        bc_proj.reshape(nb, sub, bc_cols),
        dt_proj.reshape(nb, sub, heads),
        a_rate[None],
        dt_bias[None],
        d_skip[None],
        conv_x_weight,
        conv_bc_weight,
        norm_gain[None],
        out_weight,
    )
    return (
        mixed[None],
        ssm.reshape(1, 1, heads, piece * NSTATE),
        tail_x[None, None],
        tail_bc[None, None],
    )


def either(sizes, x_proj, *rest):
    n, n_head, n_rep = sizes["seq"], sizes["head"], sizes["rep"]
    nb, sub, channels = x_proj.shape[1], x_proj.shape[3], x_proj.shape[4]
    fits = (
        nb * sub == SPAN
        and nb == n
        and sub % 16 == 0
        and n_head == n_rep
        and channels % (n * LANES) == 0
        and rest[9].shape[0] * n == channels
    )
    return fused(sizes, x_proj, *rest) if fits else local(x_proj, *rest)


def solution(mesh):
    return jax.shard_map(
        functools.partial(either, dict(mesh.shape)),
        mesh=mesh,
        in_specs=(
            P(("grp", "rep"), None, "seq", None, "head"),
            P(("grp", "rep"), None, "seq", None, "head"),
            P(("grp", "rep"), None, "seq", None, None),
            P(("grp", "rep"), None, "seq", None, "head"),
            P("head"),
            P("head"),
            P("head"),
            P(None, "head"),
            P(),
            P("head"),
            P(("seq", "rep"), "head"),
            P(("grp", "rep")),
            P(("grp", "rep"), None),
        ),
        out_specs=(
            P(("grp", "rep"), "seq", "head"),
            P(("grp", "rep"), "seq", "head", None),
            P(("grp", "rep"), "seq", None, "head"),
            P(("grp", "rep"), "seq", None, None),
        ),
        check_vma=False,
    )
```

```python
import functools

import jax
import jax.numpy as jnp
from jax import lax
from jax.experimental import pallas as pl
from jax.experimental.pallas import tpu as pltpu
from jax.sharding import PartitionSpec as P

HEAD_DIM = 64
NSTATE = 128
KCONV = 4
SPAN = 128
INNER = 8192


highest = lax.Precision.HIGHEST
stability_constant = 1e-05


def passed_along(value, axis, by):
    devices = lax.axis_size(axis)
    pairs = [(i, i + by) for i in range(devices) if 0 <= i + by < devices]
    return lax.ppermute(value, axis, pairs)


def prefix(value, axis, combine, identity, reverse):
    devices, place = (lax.axis_size(axis), lax.axis_index(axis))
    everything = jax.tree.map(lambda part: lax.all_gather(part, axis), value)
    start = jax.tree.map(
        lambda part, zero: jnp.broadcast_to(jnp.asarray(zero, part.dtype), part.shape),
        value,
        identity,
    )

    def lap(k, before):
        at = devices - 1 - k if reverse else k
        reached = at > place if reverse else at < place
        new = combine(before, jax.tree.map(lambda part: part[at], everything))
        return jax.tree.map(lambda a, b: jnp.where(reached, a, b), new, before)

    return lax.fori_loop(0, devices, lap, start)


def broadcast(block, axis, source):
    block = jnp.where(lax.axis_index(axis) == source, block, jnp.zeros_like(block))
    return lax.psum(block, axis)


def span_terms(x_conv, b_rows, c_rows, step_size, log_decay):
    cum_decay = jnp.cumsum(log_decay, axis=1)
    scores = jnp.einsum("kqn,ktn->kqt", c_rows, b_rows, preferred_element_type=jnp.float32)
    cum_heads = jnp.swapaxes(cum_decay, 1, 2)
    step_heads = jnp.swapaxes(step_size, 1, 2)
    block_len = cum_decay.shape[1]
    causal = jnp.arange(block_len)[:, None] >= jnp.arange(block_len)[None, :]
    decay_gap = cum_heads[:, :, :, None] - cum_heads[:, :, None, :]
    seg_decay = jnp.exp(jnp.where(causal, decay_gap, -jnp.inf))
    weights = (scores[:, None] * seg_decay * step_heads[:, :, None, :]).astype(jnp.bfloat16)
    y_intra = jnp.einsum("khqt,kthp->kqhp", weights, x_conv, preferred_element_type=jnp.float32)
    remaining_length = jnp.exp(cum_decay[:, -1:, :] - cum_decay)
    scaled = ((remaining_length * step_size)[..., None] * x_conv.astype(jnp.float32)).astype(
        jnp.bfloat16
    )
    states = jnp.einsum("kthp,ktn->khpn", scaled, b_rows, preferred_element_type=jnp.float32)
    return (cum_decay, y_intra, states, jnp.exp(cum_decay[:, -1, :]))


def conv_silu(preceding_tokens, current, weight):
    extended = jnp.concatenate([preceding_tokens, current], axis=0)
    length = current.shape[0]
    accum = jnp.zeros(current.shape, jnp.float32)
    for offset in range(weight.shape[0]):
        accum = accum + weight[offset] * extended[offset : offset + length].astype(jnp.float32)
    return jax.nn.silu(accum)


def link(preceding_tokens, later):
    return (
        preceding_tokens[0] * later[0],
        later[0][:, None, None] * preceding_tokens[1] + later[1],
    )


def multiply(preceding_tokens, later):
    return preceding_tokens * later


def add_rows(source, piece):
    return jnp.dot(source, piece, preferred_element_type=jnp.float32)


def take_slab(values, slab_index, seq_count):
    grouped = values.reshape(values.shape[0], seq_count, -1)
    return lax.dynamic_index_in_dim(grouped, slab_index, axis=1, keepdims=False)


def local(
    x_proj,
    gate_proj,
    bc_proj,
    dt_proj,
    a_rate,
    dt_bias,
    d_skip,
    conv_x_weight,
    conv_bc_weight,
    norm_gain,
    out_weight,
    request_first_position,
    owner,
):
    x_all, z_all, bc_all, dt_all = (
        lax.all_to_all(x_proj, "seq", split_axis=1, concat_axis=2, tiled=True),
        lax.all_to_all(gate_proj, "seq", split_axis=1, concat_axis=2, tiled=True),
        lax.all_to_all(bc_proj, "seq", split_axis=1, concat_axis=2, tiled=True),
        lax.all_to_all(dt_proj, "seq", split_axis=1, concat_axis=2, tiled=True),
    )
    tokens_here = x_all.shape[2] * x_all.shape[3]
    x_local = x_all.reshape(tokens_here, x_all.shape[4])
    z_local = z_all.reshape(tokens_here, z_all.shape[4])
    bc_local = bc_all.reshape(tokens_here, bc_all.shape[4])
    dt_local = dt_all.reshape(tokens_here, dt_all.shape[4])
    heads = dt_local.shape[1]
    seq_index = lax.axis_index("seq")
    seq_count = lax.axis_size("seq")
    positions = seq_index * tokens_here + jnp.arange(tokens_here, dtype=jnp.int32)
    is_live = positions >= request_first_position[0]
    x_live = jnp.where(is_live[:, None], x_local, jnp.zeros_like(x_local))
    bc_live = jnp.where(is_live[:, None], bc_local, jnp.zeros_like(bc_local))
    rim_rows = KCONV - 1
    tail_x = x_live[tokens_here - rim_rows :]
    tail_bc = bc_live[tokens_here - rim_rows :]
    before_x, before_bc = passed_along((tail_x, tail_bc), "seq", 1)
    x_conv = conv_silu(before_x, x_live, conv_x_weight).astype(jnp.bfloat16)
    bc_conv = conv_silu(before_bc, bc_live, conv_bc_weight).astype(jnp.bfloat16)
    step_size = (
        jax.nn.softplus(dt_local.astype(jnp.float32) + dt_bias)
        * is_live.astype(jnp.float32)[:, None]
    )
    log_decay = -a_rate * step_size
    blocks = tokens_here // SPAN
    x_blocks = x_conv.reshape(blocks, SPAN, heads, HEAD_DIM)
    b_blocks = bc_conv[:, :NSTATE].reshape(blocks, SPAN, NSTATE)
    c_blocks = bc_conv[:, NSTATE:].reshape(blocks, SPAN, NSTATE)
    cum_decay, y_intra, states, decays = span_terms(
        x_blocks,
        b_blocks,
        c_blocks,
        step_size.reshape(blocks, SPAN, heads),
        log_decay.reshape(blocks, SPAN, heads),
    )

    def advance(carry, inputs):
        factor, contrib = inputs
        return (factor[:, None, None] * carry + contrib, carry)

    zero_state = jnp.zeros((heads, HEAD_DIM, NSTATE), jnp.float32)
    local_final, local_enter = lax.scan(advance, zero_state, (decays, states))
    dev_decay = jnp.prod(decays, axis=0)
    ones_heads = jnp.ones((heads,), jnp.float32)
    enter_decay, enter_state = prefix(
        (dev_decay, local_final), "seq", link, (ones_heads, zero_state), False
    )
    c_wide = c_blocks.astype(jnp.float32)
    before_block = jnp.concatenate([ones_heads[None], jnp.cumprod(decays, axis=0)[:-1]], axis=0)
    entering = local_enter + before_block[:, :, None, None] * enter_state[None]
    y_state = jnp.exp(cum_decay)[..., None] * jnp.einsum(
        "kqn,khpn->kqhp", c_wide, entering, precision=highest
    )
    y_total = y_intra + y_state + d_skip[:, None] * x_blocks.astype(jnp.float32)
    y_flat = y_total.reshape(tokens_here, heads * HEAD_DIM)
    gated = y_flat * jax.nn.silu(z_local.astype(jnp.float32))
    square_sums = lax.psum(jnp.sum(gated * gated, axis=1), "head")
    normed = (
        gated * lax.rsqrt(square_sums[:, None] / INNER + stability_constant) * norm_gain
    ).astype(jnp.bfloat16)
    last_index = seq_count - 1
    after_decay = prefix(dev_decay, "seq", multiply, ones_heads, True)
    final_state = lax.psum(after_decay[:, None, None] * local_final, "seq")
    keep_x, keep_bc = (broadcast(tail_x, "seq", last_index), broadcast(tail_bc, "seq", last_index))
    slab_index = jnp.sum(
        jnp.where(owner[0] == seq_index, jnp.arange(seq_count, dtype=jnp.int32), 0)
    )
    ssm_state = take_slab(final_state.reshape(heads, -1), slab_index, seq_count)[None, None]
    conv_x_state = take_slab(keep_x, slab_index, seq_count)[None, None]
    conv_bc_state = take_slab(keep_bc, slab_index, seq_count)[None, None]
    features = lax.all_gather(normed, "head", axis=1, tiled=True)
    out_cols = out_weight.shape[1]
    mixed_sum = add_rows(features, lax.all_gather(out_weight, ("seq", "rep"), axis=0, tiled=True))
    mixed = mixed_sum.astype(jnp.bfloat16).reshape(1, tokens_here, out_cols)
    return (mixed, ssm_state, conv_x_state, conv_bc_state)


MESH = pl.DeviceIdType.MESH
LANES = 128
PAD = 8
F32 = jnp.float32
BF16 = jnp.bfloat16
NT = (((1,), (1,)), ((), ()))
TN = (((0,), (0,)), ((), ()))


def split3(value):
    hi = value.astype(BF16)
    rest = value - hi.astype(F32)
    mid = rest.astype(BF16)
    return hi, mid, (rest - mid.astype(F32)).astype(BF16)


def pick(parts, chosen):
    return sum(jnp.dot(parts[k], chosen, preferred_element_type=F32) for k in range(3))


def silu(value):
    return value * (1.0 / (1.0 + jnp.exp(-value)))


def fused_kernel(
    sizes,
    start_ref, owner_ref, x_ref, z_ref, bc_ref, dt_ref, rate_ref, bias_ref, skip_ref,
    cw_ref, cbw_ref, gain_ref, w_ref,
    mixed_ref, ssm_ref, tailx_ref, tailbc_ref,
    xs, zs, bcs, dts, xpad, bpad, b_scr, c_scr, cum3, step3, rows_t, scores, y_scr, g_scr,
    fin, fsnd, frecv, tails, wfull, psnd, precv, pown, qsnd, qrecv, ssnd, srecv,
    sx, rx, sz, rz, sb, rb, sd, rd, sw, rw, swf, rwf, st, rt, sf, rf, sp, rp, sq, rq, ss, rs,
):
    n_grp, n, n_head, n_rep = (sizes[a] for a in ("grp", "seq", "head", "rep"))
    me, head = lax.axis_index("seq"), lax.axis_index("head")
    grp, rep = lax.axis_index("grp"), lax.axis_index("rep")
    nb, _, sub, width = xs.shape
    length = nb * n * sub
    blocks = length // SPAN
    heads = dt_ref.shape[2]
    own_heads = heads // n
    out_cols = w_ref.shape[1]

    def exchange(src_of, dst_of, send, recv):
        copies = []
        for o in range(1, n):
            to = lax.rem(me + o, n)
            copies.append(pltpu.make_async_remote_copy(
                src_ref=src_of(to), dst_ref=dst_of, send_sem=send.at[o], recv_sem=recv.at[o],
                device_id={"seq": to}, device_id_type=MESH))
        own = pltpu.make_async_copy(src_of(me), dst_of, recv.at[0])
        for copy in copies:
            copy.start()
        own.start()
        return copies + [own]

    def cols(j):
        return pl.ds(pl.multiple_of(j * width, LANES), width)

    bc_copies = exchange(lambda j: bc_ref, bcs.at[:, me], sb, rb)
    dt_copies = exchange(lambda j: dt_ref, dts.at[:, me], sd, rd)

    x_copies = exchange(lambda j: x_ref.at[:, :, cols(j)], xs.at[:, me], sx, rx)

    w_rows = w_ref.shape[0] // n_grp
    part = me * n_rep + rep
    to_seq, to_head, to_rep = lax.rem(part, n), part // n, head
    w_self = (to_seq == me) & (to_head == head) & (to_rep == rep)

    def w_piece(g, c):
        return wfull.at[pl.ds(pl.multiple_of(g * w_rows, 16), w_rows),
                        pl.ds(pl.multiple_of(c * out_cols, LANES), out_cols)]

    w_src = w_ref.at[pl.ds(pl.multiple_of(grp * w_rows, 16), w_rows), :]
    w_copy = pltpu.make_async_remote_copy(
        src_ref=w_src, dst_ref=w_piece(grp, head), send_sem=sw, recv_sem=rw,
        device_id={"seq": to_seq, "head": to_head, "rep": to_rep}, device_id_type=MESH)

    @pl.when(w_self)
    def _():
        pltpu.make_async_copy(w_src, w_piece(grp, head), rw).start()

    @pl.when(jnp.logical_not(w_self))
    def _():
        w_copy.start()

    z_copies = exchange(lambda j: z_ref.at[:, :, cols(j)], zs.at[:, me], sz, rz)

    begin = start_ref[0]
    live = lax.broadcasted_iota(jnp.int32, (length, LANES), 0) >= begin
    row_id = lax.broadcasted_iota(jnp.int32, (SPAN, SPAN), 0)
    col_id = lax.broadcasted_iota(jnp.int32, (SPAN, SPAN), 1)
    causal = row_id >= col_id
    head_row = lax.broadcasted_iota(jnp.int32, (heads, LANES), 0)
    lane_head = lax.broadcasted_iota(jnp.int32, (heads, LANES), 1) // HEAD_DIM
    per_chunk = LANES // HEAD_DIM

    for copy in bc_copies + dt_copies:
        copy.wait()

    bpad[0:PAD, :] = jnp.zeros((PAD, bpad.shape[1]), F32)
    xpad[0:PAD, :] = jnp.zeros((PAD, LANES), F32)
    for half, target in ((0, b_scr), (1, c_scr)):
        at = pl.ds(half * NSTATE, NSTATE)
        bv = bcs[:, :, :, at].reshape(length, NSTATE).astype(F32)
        bpad[PAD:, at] = jnp.where(live, bv, 0.0)
        acc = jnp.zeros((length, NSTATE), F32)
        for k in range(KCONV):
            acc = acc + cbw_ref[k : k + 1, at] * bpad[pl.ds(PAD - KCONV + 1 + k, length), at]
        target[...] = silu(acc).astype(BF16)

    d = dts[...].reshape(length, heads).astype(F32) + bias_ref[...]
    step = jnp.maximum(d, 0.0) + jnp.log1p(jnp.exp(-jnp.abs(d)))
    step = jnp.where(live[:, :heads], step, 0.0)
    decay = -rate_ref[...] * step
    lower = causal.astype(F32)
    eye = (lax.broadcasted_iota(jnp.int32, (heads, heads), 0)
           == lax.broadcasted_iota(jnp.int32, (heads, heads), 1)).astype(F32)
    for c in range(blocks):
        r = slice(c * SPAN, (c + 1) * SPAN)
        cum = jnp.dot(lower, decay[r], precision=highest, preferred_element_type=F32)
        for k, (a, b) in enumerate(zip(split3(cum), split3(step[r]))):
            cum3[k, r, :] = a
            step3[k, r, :] = b
        rows_t[0, c] = lax.dot_general(eye, cum, NT, precision=highest, preferred_element_type=F32)
        rows_t[1, c] = lax.dot_general(eye, step[r], NT, precision=highest, preferred_element_type=F32)
        raw = lax.dot_general(c_scr[r, :], b_scr[r, :], NT, preferred_element_type=F32)
        scores[c] = jnp.where(causal, raw, 0.0)

    for copy in x_copies:
        copy.wait()
    tail_src = xs.at[nb - 1, n - 1, sub - 16 : sub, :]
    t_copies = exchange(lambda j: tail_src, tails.at[me], st, rt)

    left = lax.broadcasted_iota(jnp.int32, (SPAN, LANES), 1) < HEAD_DIM

    def chunk(i):
        lanes = pl.ds(pl.multiple_of(i * LANES, LANES), LANES)
        wide = pl.ds(pl.multiple_of(me * width + i * LANES, LANES), LANES)
        xv = xs[:, :, :, lanes].reshape(length, LANES).astype(F32)
        xpad[PAD:, :] = jnp.where(live, xv, 0.0)
        acc = jnp.zeros((length, LANES), F32)
        for k in range(KCONV):
            acc = acc + cw_ref[k : k + 1, wide] * xpad[pl.ds(PAD - KCONV + 1 + k, length), :]
        xc = silu(acc).astype(BF16)
        first = me * own_heads + i * per_chunk
        chosen_f = (head_row == first + lane_head).astype(F32)
        chosen = chosen_f.astype(BF16)
        cum_l = pick(cum3, chosen)
        step_l = pick(step3, chosen)
        skip = jnp.dot(jnp.broadcast_to(skip_ref[...], (8, heads)), chosen_f, precision=highest,
                       preferred_element_type=F32)[0:1]
        state = jnp.zeros((NSTATE, LANES), F32)
        for c in range(blocks):
            r = slice(c * SPAN, (c + 1) * SPAN)
            cl, sl, xb = cum_l[r], step_l[r], xc[r]
            y = skip * xb.astype(F32)
            for k in range(per_chunk):
                cum_q = jnp.broadcast_to(cl[:, k * HEAD_DIM : k * HEAD_DIM + 1], (SPAN, SPAN))
                cum_t = rows_t[0, c, pl.ds(first + k, 1), :]
                step_t = rows_t[1, c, pl.ds(first + k, 1), :]
                mix = (scores[c] * jnp.exp(jnp.minimum(cum_q - cum_t, 0.0)) * step_t).astype(BF16)
                xk = jnp.where(left if k == 0 else jnp.logical_not(left), xb.astype(F32), 0.0).astype(BF16)
                y = y + jnp.dot(mix, xk, preferred_element_type=F32)
            if c:
                y = y + jnp.exp(cl) * jnp.dot(c_scr[r, :], state.astype(BF16), preferred_element_type=F32)
            y_scr[r, lanes] = y
            last = cl[SPAN - 1 : SPAN, :]
            scaled = (jnp.exp(last - cl) * sl * xb.astype(F32)).astype(BF16)
            state = jnp.exp(last) * state + lax.dot_general(
                b_scr[r, :], scaled, TN, preferred_element_type=F32)
        turned = state.T
        piece = HEAD_DIM // n
        for k in range(per_chunk):
            for p in range(HEAD_DIM):
                fin[p // piece, p % piece, pl.ds(i * per_chunk + k, 1), :] = (
                    turned[k * HEAD_DIM + p : k * HEAD_DIM + p + 1, :])

    half = width // LANES // 2
    pl.loop(0, half)(chunk)

    @pl.when(w_self)
    def _():
        pltpu.make_async_copy(w_src, w_piece(grp, head), rw).wait()

    @pl.when(jnp.logical_not(w_self))
    def _():
        w_copy.wait()

    def forward(piece_grp, og, orr, to):
        slot = og * n_rep + orr
        piece = w_piece(piece_grp, rep)
        return pltpu.make_async_remote_copy(
            src_ref=piece, dst_ref=piece, send_sem=swf.at[slot], recv_sem=rwf.at[slot],
            device_id=to, device_id_type=MESH)

    over_grp = [forward(grp, og, 0, {"grp": lax.rem(grp + og, n_grp)}) for og in range(1, n_grp)]
    over_rep = [forward(grp, 0, o, {"rep": lax.rem(rep + o, n_rep)}) for o in range(1, n_rep)]
    for copy in over_grp + over_rep:
        copy.start()

    pl.loop(half, width // LANES)(chunk)

    for copy in over_grp:
        copy.wait()
    again = [
        forward(lax.rem(grp + n_grp - og, n_grp), og, o, {"rep": lax.rem(rep + o, n_rep)})
        for og in range(1, n_grp)
        for o in range(1, n_rep)
    ]
    for copy in again:
        copy.start()

    def slab_of(s):
        return jnp.minimum(sum(jnp.where(owner_ref[j] == s, j, 0) for j in range(n)), n - 1)

    f_copies = []
    for o in range(1, n):
        to = lax.rem(me + o, n)
        fsnd[o] = fin[slab_of(to)].astype(BF16)
        f_copies.append(pltpu.make_async_remote_copy(
            src_ref=fsnd.at[o], dst_ref=frecv.at[me], send_sem=sf.at[o], recv_sem=rf.at[o],
            device_id={"seq": to}, device_id_type=MESH))
        f_copies[-1].start()

    for copy in z_copies:
        copy.wait()

    def gate_chunk(i, total):
        lanes = pl.ds(pl.multiple_of(i * LANES, LANES), LANES)
        wide = pl.ds(pl.multiple_of(me * width + i * LANES, LANES), LANES)
        zv = zs[:, :, :, lanes].reshape(length, LANES).astype(F32)
        gated = y_scr[:, lanes] * silu(zv)
        g_scr[:, lanes] = (gated * gain_ref[:, wide]).astype(BF16)
        return total + gated * gated

    squares = lax.fori_loop(0, width // LANES, gate_chunk, jnp.zeros((length, LANES), F32))
    for c in range(blocks):
        r = slice(c * SPAN, (c + 1) * SPAN)
        total = jnp.broadcast_to(jnp.sum(squares[r], axis=1, keepdims=True), (SPAN, LANES))
        ssnd[c] = total.T[0:8, :]

    s_copies = []
    for oh in range(n_head):
        for o in range(n):
            if oh or o:
                to = lax.rem(me + o, n)
                slot = oh * n + o
                s_copies.append(pltpu.make_async_remote_copy(
                    src_ref=ssnd.at[to], dst_ref=srecv.at[slot], send_sem=ss.at[slot],
                    recv_sem=rs.at[slot],
                    device_id={"seq": to, "head": lax.rem(head + oh, n_head)}, device_id_type=MESH))
    for copy in s_copies:
        copy.start()
    for copy in over_rep + again:
        copy.wait()

    tile = 256 if out_cols % 256 == 0 else LANES

    def product(h, put):
        @pl.loop(0, out_cols // tile)
        def _(i):
            at = pl.ds(pl.multiple_of(h * out_cols + i * tile, LANES), tile)
            out = jnp.dot(g_scr[...], wfull[:, at], preferred_element_type=F32)
            put(pl.ds(pl.multiple_of(i * tile, LANES), tile), out.reshape(blocks, SPAN, tile))

    p_copies = {}
    for oh in range(1, n_head):
        to_h = lax.rem(head + oh, n_head)

        def put(at, out, oh=oh):
            psnd[oh - 1, :, :, at] = out.astype(BF16)

        product(to_h, put)
        for o in [*range(1, n), 0]:
            block = lax.rem(me + o, n)
            p_copies[oh, o] = pltpu.make_async_remote_copy(
                src_ref=psnd.at[oh - 1, block], dst_ref=precv.at[oh - 1, block],
                send_sem=sp.at[oh - 1, o], recv_sem=rp.at[oh - 1, o],
                device_id={"head": to_h}, device_id_type=MESH)
            p_copies[oh, o].start()

    def put_own(at, out):
        pown[:, :, at] = out

    product(head, put_own)

    q_copies = []
    for o in [*range(1, n), 0]:
        block = lax.rem(me + o, n)
        whole = pown[block]
        for oh in range(1, n_head):
            p_copies[oh, o].wait()
            whole = whole + precv[oh - 1, block].astype(F32)
        if o:
            qsnd[o] = whole.astype(BF16)
            q_copies.append(pltpu.make_async_remote_copy(
                src_ref=qsnd.at[o], dst_ref=qrecv.at[o], send_sem=sq.at[o], recv_sem=rq.at[o],
                device_id={"seq": block}, device_id_type=MESH))
            q_copies[-1].start()
        else:
            pown[block] = whole

    for copy in s_copies + t_copies:
        copy.wait()
    total = ssnd[me]
    for slot in range(1, n * n_head):
        total = total + srecv[slot]
    scale_row = lax.rsqrt(total / INNER + stability_constant)
    scale = jnp.broadcast_to(scale_row[0:1], (SPAN, LANES)).T

    slab = slab_of(me)
    tail_live = length - 16 + lax.broadcasted_iota(jnp.int32, (16, width), 0) >= begin
    rim = KCONV - 1
    kept = jnp.where(tail_live, tails[slab].astype(F32), 0.0)
    tailx_ref[...] = kept[16 - rim :].astype(BF16)
    state_cols = tailbc_ref.shape[1]
    wide_bc = bcs.shape[3]
    chosen = (lax.broadcasted_iota(jnp.int32, (wide_bc, state_cols), 0)
              == slab * state_cols + lax.broadcasted_iota(jnp.int32, (wide_bc, state_cols), 1)).astype(BF16)
    kept = jnp.dot(
        bpad[PAD + length - 16 : PAD + length, :].astype(BF16), chosen, preferred_element_type=F32)
    tailbc_ref[...] = kept[16 - rim :].astype(BF16)

    for copy in f_copies:
        copy.wait()
    for o in range(n):
        source = lax.rem(me + n - o, n)
        for p in range(HEAD_DIM // n):
            value = frecv[source, p].astype(F32) if o else fin[slab, p]
            ssm_ref[source, :, p * NSTATE : (p + 1) * NSTATE] = value

    for copy in q_copies:
        copy.wait()
    for at in range(0, out_cols, LANES):
        lanes = slice(at, at + LANES)
        whole = pown[me, :, lanes]
        for o in range(1, n):
            whole = whole + qrecv[o, :, lanes].astype(F32)
        mixed_ref[:, lanes] = (whole * scale).astype(BF16)


def fused(
    sizes, x_proj, gate_proj, bc_proj, dt_proj, a_rate, dt_bias, d_skip, conv_x_weight,
    conv_bc_weight, norm_gain, out_weight, request_first_position, owner,
):
    n_grp, n, n_head, n_rep = (sizes[a] for a in ("grp", "seq", "head", "rep"))
    nb, sub, channels = x_proj.shape[1], x_proj.shape[3], x_proj.shape[4]
    heads, bc_cols = dt_proj.shape[4], bc_proj.shape[4]
    length, width = nb * n * sub, channels // n
    blocks, own_heads, out_cols = length // SPAN, heads // n, out_weight.shape[1]
    piece = HEAD_DIM // n
    vmem = lambda shape, kind: pltpu.VMEM(shape, kind)
    dma = lambda *shape: pltpu.SemaphoreType.DMA(shape)
    hbm = pl.BlockSpec(memory_space=pl.ANY)
    here = pl.BlockSpec(memory_space=pltpu.VMEM)
    smem = pl.BlockSpec(memory_space=pltpu.SMEM)
    mixed, ssm, tail_x, tail_bc = pl.pallas_call(
        functools.partial(fused_kernel, sizes),
        out_shape=(
            jax.ShapeDtypeStruct((SPAN, out_cols), BF16),
            jax.ShapeDtypeStruct((n, own_heads, piece * NSTATE), F32),
            jax.ShapeDtypeStruct((KCONV - 1, width), BF16),
            jax.ShapeDtypeStruct((KCONV - 1, bc_cols // n), BF16),
        ),
        in_specs=[smem, smem, hbm, hbm, hbm, hbm] + [here] * 6 + [hbm],
        out_specs=(here,) * 4,
        scratch_shapes=[
            vmem((nb, n, sub, width), BF16),
            vmem((nb, n, sub, width), BF16),
            vmem((nb, n, sub, bc_cols), BF16),
            vmem((nb, n, sub, heads), BF16),
            vmem((length + PAD, LANES), F32),
            vmem((length + PAD, bc_cols), F32),
            vmem((length, NSTATE), BF16),
            vmem((length, NSTATE), BF16),
            vmem((3, length, heads), BF16),
            vmem((3, length, heads), BF16),
            vmem((2, blocks, heads, SPAN), F32),
            vmem((blocks, SPAN, SPAN), F32),
            vmem((length, width), F32),
            vmem((length, width), BF16),
            vmem((n, piece, own_heads, NSTATE), F32),
            vmem((n, piece, own_heads, NSTATE), BF16),
            vmem((n, piece, own_heads, NSTATE), BF16),
            vmem((n, 16, width), BF16),
            vmem((width, out_cols * n_head), BF16),
            vmem((n_head - 1, blocks, SPAN, out_cols), BF16),
            vmem((n_head - 1, blocks, SPAN, out_cols), BF16),
            vmem((blocks, SPAN, out_cols), F32),
            vmem((n, SPAN, out_cols), BF16),
            vmem((n, SPAN, out_cols), BF16),
            vmem((blocks, 8, LANES), F32),
            vmem((n * n_head, 8, LANES), F32),
            dma(n), dma(n), dma(n), dma(n), dma(n), dma(n), dma(n), dma(n),
            pltpu.SemaphoreType.DMA, pltpu.SemaphoreType.DMA,
            dma(n_grp * n_rep), dma(n_grp * n_rep),
            dma(n), dma(n), dma(n), dma(n),
            dma(n_head - 1, n), dma(n_head - 1, n),
            dma(n), dma(n), dma(n * n_head), dma(n * n_head),
        ],
        compiler_params=pltpu.CompilerParams(
            has_side_effects=True, vmem_limit_bytes=56 * 1024 * 1024
        ),
    )(
        request_first_position,
        owner.reshape(n),
        x_proj.reshape(nb, sub, channels),
        gate_proj.reshape(nb, sub, channels),
        bc_proj.reshape(nb, sub, bc_cols),
        dt_proj.reshape(nb, sub, heads),
        a_rate[None],
        dt_bias[None],
        d_skip[None],
        conv_x_weight,
        conv_bc_weight,
        norm_gain[None],
        out_weight,
    )
    return (
        mixed[None],
        ssm.reshape(1, 1, heads, piece * NSTATE),
        tail_x[None, None],
        tail_bc[None, None],
    )


def either(sizes, x_proj, *rest):
    n, n_head, n_rep = sizes["seq"], sizes["head"], sizes["rep"]
    nb, sub, channels = x_proj.shape[1], x_proj.shape[3], x_proj.shape[4]
    fits = (
        nb * sub == SPAN
        and nb == n
        and sub % 16 == 0
        and n_head == n_rep
        and channels % (n * LANES) == 0
        and rest[9].shape[0] * n == channels
    )
    return fused(sizes, x_proj, *rest) if fits else local(x_proj, *rest)


def solution(mesh):
    return jax.shard_map(
        functools.partial(either, dict(mesh.shape)),
        mesh=mesh,
        in_specs=(
            P(("grp", "rep"), None, "seq", None, "head"),
            P(("grp", "rep"), None, "seq", None, "head"),
            P(("grp", "rep"), None, "seq", None, None),
            P(("grp", "rep"), None, "seq", None, "head"),
            P("head"),
            P("head"),
            P("head"),
            P(None, "head"),
            P(),
            P("head"),
            P(("seq", "rep"), "head"),
            P(("grp", "rep")),
            P(("grp", "rep"), None),
        ),
        out_specs=(
            P(("grp", "rep"), "seq", "head"),
            P(("grp", "rep"), "seq", "head", None),
            P(("grp", "rep"), "seq", None, "head"),
            P(("grp", "rep"), "seq", None, None),
        ),
        check_vma=False,
    )
```
